32 devices in a mesh: row: 16 (over z, y, core), col: 2 (over x).
Axes of the slice: x: 2, y: 2, z: 4, core: 2. Of those that a mesh axis runs over, the one named last changes fastest.
Arguments:
- inputs: bfloat16 [1536, 1024], P(('row', 'col')), may hold values from -6 to 6
- first_weight: bfloat16 [1024, 1024], replicated, may hold values from -0.1875 to 0.1875
- second_weight: bfloat16 [1024, 1024], replicated, may hold values from -0.1875 to 0.1875
- readout: bfloat16 [1024], replicated, may hold values from -0.1875 to 0.1875
- target: float32 [1536], P(('row', 'col')), may hold values from -6 to 6
- counts: int32 [1536], P(('row', 'col')), may hold values from 1 to 32, as said below
- views: int32 [1536], P(('row', 'col')), may hold values from 0 to 1999
Outputs:
- update: float32 [1024, 2048], P(('row', 'col'))
The draws below stay inside these ranges and needn't reach their ends.
Inputs may be any that keep to these rules, and one draw needn't show every extreme that they name: `counts`: number of samples taken along the ray.
All inputs are finite; a program needn't handle non-finite values.
Results may differ from the reference program's by a relative error of at most 0.008.
Values may be sent and summed in bfloat16 or wider, within the bound.
No kernel may reach another device: no remote copies, remote signals or barrier semaphores. Data moves between devices by JAX's collectives and lax.ppermute only.
A program may use at most 128 MiB of HBM per device.

```python
import jax
import jax.numpy as jnp
from jax import lax

D = 1024
VIEWS = 2000
ITERS = 3
ROWS = 1536


def draw_counts(key, part):
    positions = jnp.arange(ROWS, dtype=jnp.int32)
    top = 9 + 24 * positions // ROWS
    return jax.random.randint(key, (ROWS,), 1, top + 1, dtype=jnp.int32)


def set_ends(result, rng, low, largest):
    place = [jax.random.randint(jax.random.fold_in(rng, axis), (), 0, length) for axis, length in enumerate(result.shape)]
    main_axis = result.shape.index(max(result.shape))
    neighbour = place[:main_axis] + [(place[main_axis] + 1) % result.shape[main_axis]] + place[main_axis + 1:]
    return result.at[tuple(place)].set(low).at[tuple(neighbour)].set(largest)


def with_spikes(drawn, rng, source, target, parts, factor):
    owner, partner = [(jnp.arange(drawn.shape[dim]) // (drawn.shape[dim] // parts)).reshape([-1 if axis == dim else 1 for axis in range(drawn.ndim)]) for dim in (source, target)]
    chosen = jax.random.permutation(rng, parts)[partner]
    strong = (owner == chosen) | (owner == (partner + parts // 2) % parts)
    return jnp.where(strong, factor * drawn, drawn)


def shard_levels(stream_key, dims, pieces, low, top_value):
    def one(dim, parts):
        draws = jax.random.uniform(jax.random.fold_in(jax.random.fold_in(stream_key, 6), dim), (parts,), jnp.float32, low / len(pieces), top_value / len(pieces))
        return jnp.repeat(jnp.exp(draws), dims[dim] // parts).reshape((-1,) + (1,) * (len(dims) - dim - 1))

    factor_of = one(*pieces[0])
    for cut in pieces[1:]:
        factor_of = factor_of * one(*cut)
    return factor_of


def centred(key, extent, scale, reach, cuts=(), kind=jnp.bfloat16):
    gain = shard_levels(key, extent, cuts, -0.22, 0.18) if cuts else 1.0
    entries = jax.random.normal(key, extent, jnp.float32) * scale * gain
    return jnp.minimum(jnp.maximum(entries, -reach), reach).astype(kind)


def heavy_noise(stream_key, extent, width, bound, shards, heavy, kind=jnp.bfloat16):
    drawn = width * jax.random.normal(stream_key, extent, jnp.float32)
    if shards:
        drawn = drawn * shard_levels(stream_key, extent, shards, -0.22, 0.18)
    return jnp.clip(with_spikes(drawn, jax.random.fold_in(stream_key, 3), *heavy), -bound, bound).astype(kind)


def setup_inputs(seed: int = 0) -> dict:
    keys = jax.random.split(jax.random.key(seed), 8)
    inputs = heavy_noise(keys[0], (ROWS, D), 1.0, 6.0, ((0, 32),), (0, 1, 32, 2.75))
    first_weight = centred(keys[1], (D, D), D ** -0.5, 0.1875)
    second_weight = centred(keys[2], (D, D), D ** -0.5, 0.1875)
    readout = centred(keys[3], (D,), D ** -0.5, 0.1875)
    target = centred(keys[4], (ROWS,), 1.0, 6.0, ((0, 32),), jnp.float32)
    counts = draw_counts(jax.random.fold_in(keys[7], 71), 0)
    views = set_ends(jax.random.randint(keys[6], (ROWS,), 0, VIEWS), jax.random.fold_in(keys[6], 1), 0, VIEWS - 1).astype(jnp.int32)
    return dict(inputs=inputs, first_weight=first_weight, second_weight=second_weight, readout=readout, target=target, counts=counts, views=views)


DAMP = 4.0
LEARN = 8.0
HIGH = lax.Precision.HIGHEST


def slope(value):
    sig = jax.nn.sigmoid(value)
    return sig * (1.0 + value * (1.0 - sig))


def ray_weight(counts, views):
    angle = (2.0 * jnp.pi / VIEWS) * views.astype(jnp.float32)
    return counts.astype(jnp.float32) / 16.0 * (1.0 + 0.5 * jnp.cos(angle))


def reference(inputs, first_weight, second_weight, readout, target, counts, views):
    weight_rows = ray_weight(counts, views)
    pre_first = jnp.dot(inputs, first_weight, preferred_element_type=jnp.float32)
    hidden = jax.nn.silu(pre_first).astype(jnp.bfloat16)
    pre_second = jnp.dot(hidden, second_weight, preferred_element_type=jnp.float32)
    readout_f = readout.astype(jnp.float32)
    signal = jnp.sum(jax.nn.silu(pre_second) * readout_f[None, :], axis=1)
    right = weight_rows * signal - target
    outer_grad = (weight_rows[:, None] * slope(pre_second) * readout_f[None, :]).astype(jnp.bfloat16)
    carried = lax.dot_general(outer_grad, second_weight, (((1,), (1,)), ((), ())), preferred_element_type=jnp.float32)
    inner_grad = (carried * slope(pre_first)).astype(jnp.bfloat16)
    in_f = inputs.astype(jnp.float32)
    hid_f = hidden.astype(jnp.float32)
    inner_f = inner_grad.astype(jnp.float32)
    outer_f = outer_grad.astype(jnp.float32)

    def apply(direction):
        first = jnp.dot(in_f.T, direction[:, None] * inner_f, precision=HIGH)
        second = jnp.dot(hid_f.T, direction[:, None] * outer_f, precision=HIGH)
        total = jnp.sum(jnp.dot(in_f, first, precision=HIGH) * inner_f, axis=1)
        total = total + jnp.sum(jnp.dot(hid_f, second, precision=HIGH) * outer_f, axis=1)
        return total + DAMP * direction

    solution = jnp.zeros_like(right)
    residual, direction = right, right
    norm_now = jnp.sum(residual * residual)
    for step in range(ITERS):
        image = apply(direction)
        alpha = norm_now / jnp.sum(direction * image)
        solution = solution + alpha * direction
        residual = residual - alpha * image
        norm_next = jnp.sum(residual * residual)
        direction = residual + (norm_next / norm_now) * direction
        norm_now = norm_next
    first = jnp.dot(in_f.T, solution[:, None] * inner_f, precision=HIGH)
    second = jnp.dot(hid_f.T, solution[:, None] * outer_f, precision=HIGH)
    return -LEARN * jnp.concatenate([first, second], axis=1)
```

```python
import jax
import jax.numpy as jnp
from jax import lax
from jax.experimental import pallas as pl
from jax.experimental.pallas import tpu as pltpu
from jax.sharding import PartitionSpec as P

VIEWS = 2000
ITERS = 3


DAMP = 4.0
LEARN = 8.0
HIGH = lax.Precision.HIGHEST
LANES = 128
SUB = 128
VMEM_BYTES = 56 * 2**20


def slope(value):
    sig = jax.nn.sigmoid(value)
    return sig * (1.0 + value * (1.0 - sig))


def ray_weight(counts, views):
    angle = 2.0 * jnp.pi / VIEWS * views.astype(jnp.float32)
    return counts.astype(jnp.float32) / 16.0 * (1.0 + 0.5 * jnp.cos(angle))


def carry_back(outer_grad, second_weight, pre_first):
    carried = lax.dot_general(
        outer_grad, second_weight, (((1,), (1,)), ((), ())), preferred_element_type=jnp.float32
    )
    return (carried * slope(pre_first)).astype(jnp.bfloat16)


def gram(left, other):
    return lax.dot_general(
        left, other, (((1,), (1,)), ((), ())), preferred_element_type=jnp.float32
    )


def global_sums(values):
    return lax.psum((values[0], values[1]), ("row", "col"))


def shards(inputs, first_weight, second_weight, readout, target, counts, views):
    weight_rows = ray_weight(counts, views)
    pre_first = jnp.dot(inputs, first_weight, preferred_element_type=jnp.float32)
    hidden = jax.nn.silu(pre_first).astype(jnp.bfloat16)
    pre_second = jnp.dot(hidden, second_weight, preferred_element_type=jnp.float32)
    readout_f = readout.astype(jnp.float32)
    signal = jnp.sum(jax.nn.silu(pre_second) * readout_f[None, :], axis=1)
    right = weight_rows * signal - target
    outer_grad = (weight_rows[:, None] * slope(pre_second) * readout_f[None, :]).astype(
        jnp.bfloat16
    )
    inner_grad = carry_back(outer_grad, second_weight, pre_first)
    block_in, block_inner, block_hidden, block_outer = (
        lax.all_gather(inputs, "col", axis=0, tiled=True),
        lax.all_gather(inner_grad, "col", axis=0, tiled=True),
        lax.all_gather(hidden, "col", axis=0, tiled=True),
        lax.all_gather(outer_grad, "col", axis=0, tiled=True),
    )
    cross_in, cross_inner, cross_hidden, cross_outer = (
        lax.all_gather(inputs, "row", axis=0, tiled=True),
        lax.all_gather(inner_grad, "row", axis=0, tiled=True),
        lax.all_gather(hidden, "row", axis=0, tiled=True),
        lax.all_gather(outer_grad, "row", axis=0, tiled=True),
    )
    kernel = gram(block_in, cross_in) * gram(block_inner, cross_inner)
    kernel = kernel + gram(block_hidden, cross_hidden) * gram(block_outer, cross_outer)

    def apply(direction):
        spread = lax.all_gather(direction, "row", axis=0, tiled=True)
        partial_value = jnp.dot(kernel, spread, precision=HIGH, preferred_element_type=jnp.float32)
        own = lax.psum_scatter(partial_value, "col", scatter_dimension=0, tiled=True)
        return own + DAMP * direction

    solution = jnp.zeros_like(right)
    residual = right
    image = apply(residual)
    norm_now, product = global_sums((jnp.sum(residual * residual), jnp.sum(residual * image)))
    alpha = norm_now / product
    direction, along = (residual, image)
    for step in range(ITERS):
        solution = solution + alpha * direction
        residual = residual - alpha * along
        if step + 1 < ITERS:
            image = apply(residual)
            norm_next, product = global_sums(
                (jnp.sum(residual * residual), jnp.sum(residual * image))
            )
            ratio = norm_next / norm_now
            alpha = norm_next / (product - ratio * norm_next / alpha)
            direction = residual + ratio * direction
            along = image + ratio * along
            norm_now = norm_next
    weighted_inner = solution[:, None] * inner_grad.astype(jnp.float32)
    weighted_outer = solution[:, None] * outer_grad.astype(jnp.float32)
    inputs_f = inputs.astype(jnp.float32)
    hidden_f = hidden.astype(jnp.float32)
    first = lax.dot_general(
        inputs_f,
        weighted_inner,
        (((0,), (0,)), ((), ())),
        precision=HIGH,
        preferred_element_type=jnp.float32,
    )
    second = lax.dot_general(
        hidden_f,
        weighted_outer,
        (((0,), (0,)), ((), ())),
        precision=HIGH,
        preferred_element_type=jnp.float32,
    )
    return lax.psum_scatter(
        -LEARN * jnp.concatenate([first, second], axis=1),
        ("row", "col"),
        scatter_dimension=0,
        tiled=True,
    )


def split3(value):
    high = lax.reduce_precision(value, 8, 7)
    rest = value - high
    middle = lax.reduce_precision(rest, 8, 7)
    return high, middle, rest - middle


def bdot(left, right, contract):
    return lax.dot_general(left, right, (contract, ((), ())), preferred_element_type=jnp.float32)


def sigmoid(value):
    return 1.0 / (1.0 + jnp.exp(-value))


def features(rays, width, pay_ref, w1_ref, w2_ref, ro_ref, hid_ref, out_ref, inn_ref, right_ref):
    def body(i, carry):
        rows = pl.ds(pl.multiple_of(i * SUB, SUB), SUB)
        extra = pay_ref[rows, width : width + LANES].astype(jnp.float32)
        weight = extra[:, 0:1] + extra[:, 1:2] + extra[:, 2:3]
        target = extra[:, 3:4] + extra[:, 4:5] + extra[:, 5:6]
        pre = bdot(pay_ref[rows, 0:width], w1_ref[...], ((1,), (0,)))
        sig = sigmoid(pre)
        slope_first = sig * (1.0 + pre * (1.0 - sig))
        hidden = (pre * sig).astype(jnp.bfloat16)
        hid_ref[rows, :] = hidden
        pre = bdot(hidden, w2_ref[...], ((1,), (0,)))
        sig = sigmoid(pre)
        readout = ro_ref[...]
        signal = jnp.sum(pre * sig * readout, axis=1, keepdims=True)
        outer = (weight * (sig * (1.0 + pre * (1.0 - sig))) * readout).astype(jnp.bfloat16)
        out_ref[rows, :] = outer
        carried = bdot(outer, w2_ref[...], ((1,), (1,)))
        inn_ref[rows, :] = (carried * slope_first).astype(jnp.bfloat16)
        right_ref[rows, :] = jnp.broadcast_to(weight * signal - target, (SUB, LANES))
        return carry

    lax.fori_loop(0, rays // SUB, body, 0)


def products(rays, width, mine, others, strip_ref, mirror_ref):
    pay_ref, inn_ref, hid_ref, out_ref = mine

    def body(i, carry):
        rows = pl.ds(pl.multiple_of(i * SUB, SUB), SUB)
        for j, (pay_o, inn_o, hid_o, out_o) in enumerate([*others, mine]):
            nt = ((1,), (1,))
            value = bdot(pay_ref[rows, 0:width], pay_o[:, 0:width], nt) * bdot(
                inn_ref[rows, :], inn_o[...], nt
            )
            value = value + bdot(hid_ref[rows, :], hid_o[...], nt) * bdot(
                out_ref[rows, :], out_o[...], nt
            )
            strip_ref[rows, j * rays : (j + 1) * rays] = value
            if j < len(others):
                for k in range(rays // LANES):
                    mirror_ref[i, j * rays + k * LANES : j * rays + (k + 1) * LANES, :] = value[
                        :, k * LANES : (k + 1) * LANES
                    ].T
        return carry

    lax.fori_loop(0, rays // SUB, body, 0)


def stage_kernel(before, rays, width):
    def kernel(*refs):
        pay_ref, w1_ref, w2_ref, ro_ref = refs[:4]
        others = [refs[4 + 4 * j : 8 + 4 * j] for j in range(before)]
        hid_ref, out_ref, inn_ref, right_ref, strip_ref = refs[4 + 4 * before : 9 + 4 * before]
        mirror_ref = refs[9 + 4 * before] if before else None
        features(
            rays, width, pay_ref, w1_ref, w2_ref, ro_ref, hid_ref, out_ref, inn_ref, right_ref
        )
        products(rays, width, (pay_ref, inn_ref, hid_ref, out_ref), others, strip_ref, mirror_ref)

    return kernel


def stage(before, pay, w1, w2, ro, others):
    rays, width = pay.shape[0], w1.shape[0]
    units = w1.shape[1]
    vmem = pl.BlockSpec(memory_space=pltpu.VMEM)
    shapes = [jax.ShapeDtypeStruct((rays, units), jnp.bfloat16)] * 3
    shapes += [
        jax.ShapeDtypeStruct((rays, LANES), jnp.float32),
        jax.ShapeDtypeStruct((rays, rays * (before + 1)), jnp.float32),
    ]
    if before:
        shapes.append(jax.ShapeDtypeStruct((rays // SUB, rays * before, SUB), jnp.float32))
    flat = [a for four in others for a in four]
    flops = 6 * rays * width * units + 8 * rays * rays * (before + 1) * width
    return pl.pallas_call(
        stage_kernel(before, rays, width),
        out_shape=shapes,
        in_specs=[vmem] * (4 + len(flat)),
        out_specs=[vmem] * len(shapes),
        cost_estimate=pl.CostEstimate(
            flops=flops, transcendentals=4 * rays * units, bytes_accessed=8 * rays * width
        ),
        compiler_params=pltpu.CompilerParams(vmem_limit_bytes=VMEM_BYTES),
        name=f"stage{before}",
    )(pay, w1, w2, ro, *flat)


def solve_kernel(chunks, rays, width, own):
    total = chunks * rays
    tiles = total // LANES

    def kernel(*refs):
        fours = [refs[4 * j : 4 * j + 4] for j in range(chunks)]
        rights = refs[4 * chunks : 5 * chunks]
        strips = refs[5 * chunks : 6 * chunks]
        mirrors = [None, *refs[6 * chunks : 7 * chunks - 1]]
        out_ref, col_ref, res_ref = refs[7 * chunks - 1 :]
        per = rays // LANES

        def to_columns(row):
            for t in range(tiles):
                piece = jnp.broadcast_to(row[:, t * LANES : (t + 1) * LANES], (LANES, LANES))
                col_ref[t * LANES : (t + 1) * LANES, :] = piece.T

        def apply(row):
            to_columns(row)
            pieces = [None] * tiles
            for c in range(chunks):
                lower = (c + 1) * per

                def below(g, accs, c=c, lower=lower):
                    rows = pl.ds(pl.multiple_of(g * 8, 8), 8)
                    d = col_ref[pl.ds(pl.multiple_of(c * rays + g * 8, 8), 8), :]
                    return tuple(
                        a + strips[c][rows, t * LANES : (t + 1) * LANES] * d
                        for t, a in enumerate(accs)
                    )

                zeros = tuple(jnp.zeros((8, LANES), jnp.float32) for _ in range(lower))
                accs = lax.fori_loop(0, rays // 8, below, zeros, unroll=4)
                for t in range(lower):
                    pieces[t] = accs[t] if pieces[t] is None else pieces[t] + accs[t]
                if c:

                    def above(g, accs, c=c):
                        rows = pl.ds(pl.multiple_of(g * 8, 8), 8)
                        d = col_ref[rows, :]
                        return tuple(a + mirrors[c][t, rows, :] * d for t, a in enumerate(accs))

                    zeros = tuple(jnp.zeros((8, LANES), jnp.float32) for _ in range(per))
                    accs = lax.fori_loop(0, c * rays // 8, above, zeros, unroll=4)
                    for t in range(per):
                        k = c * per + t
                        pieces[k] = accs[t] if pieces[k] is None else pieces[k] + accs[t]
            joined = jnp.concatenate(pieces, axis=1)
            return jnp.sum(joined, axis=0, keepdims=True) + DAMP * row

        def dot(a, b):
            return jnp.sum(a * b, axis=1, keepdims=True)

        right = jnp.concatenate(
            [
                rights[c][k * LANES : (k + 1) * LANES, :].T[0:1, :]
                for c in range(chunks)
                for k in range(per)
            ],
            axis=1,
        )
        solution = jnp.zeros_like(right)
        residual, direction = right, right
        norm_now = dot(right, right)
        for step in range(ITERS):
            image = apply(direction)
            alpha = norm_now / dot(direction, image)
            solution = solution + alpha * direction
            if step + 1 < ITERS:
                residual = residual - alpha * image
                norm_next = dot(residual, residual)
                direction = residual + (norm_next / norm_now) * direction
                norm_now = norm_next
        to_columns(solution)
        rank = lax.axis_index("row") * lax.axis_size("col") + lax.axis_index("col")
        start = rank * own
        base = pl.multiple_of(start // LANES * LANES, LANES)
        first = jnp.zeros((LANES, width), jnp.float32)
        second = jnp.zeros((LANES, width), jnp.float32)
        tn = ((0,), (0,))
        for c, (pay_ref, inn_ref, hid_ref, grad_ref) in enumerate(fours):
            scale = col_ref[c * rays : (c + 1) * rays, :]
            for which, (a_ref, b_ref) in enumerate(((pay_ref, inn_ref), (hid_ref, grad_ref))):
                left = a_ref[:, pl.ds(base, LANES)].astype(jnp.float32) * scale
                high = left.astype(jnp.bfloat16)
                low = (left - high.astype(jnp.float32)).astype(jnp.bfloat16)
                value = bdot(high, b_ref[...], tn) + bdot(low, b_ref[...], tn)
                if which == 0:
                    first = first + value
                else:
                    second = second + value
        res_ref[:, 0:width] = first
        res_ref[:, width : 2 * width] = second
        rows = pl.ds(pl.multiple_of(start - base, own), own)
        out_ref[...] = -LEARN * res_ref[rows, :]

    return kernel


def solve(fours, rights, strips, mirrors, own):
    chunks = len(fours)
    rays, width = fours[0][1].shape
    vmem = pl.BlockSpec(memory_space=pltpu.VMEM)
    flat = [a for four in fours for a in four] + list(rights) + list(strips) + list(mirrors)
    total = chunks * rays
    return pl.pallas_call(
        solve_kernel(chunks, rays, width, own),
        out_shape=jax.ShapeDtypeStruct((own, 2 * width), jnp.float32),
        in_specs=[vmem] * len(flat),
        out_specs=vmem,
        scratch_shapes=[
            pltpu.VMEM((total, LANES), jnp.float32),
            pltpu.VMEM((LANES, 2 * width), jnp.float32),
        ],
        cost_estimate=pl.CostEstimate(
            flops=8 * LANES * total * width, transcendentals=0, bytes_accessed=8 * own * width
        ),
        compiler_params=pltpu.CompilerParams(vmem_limit_bytes=VMEM_BYTES),
        name="solve",
    )(*flat)


def gathered(inputs, first_weight, second_weight, readout, target, counts, views):
    n_row, n_col = lax.axis_size("row"), lax.axis_size("col")
    line = n_row // 4
    rays, width = inputs.shape
    weight_rows = ray_weight(counts, views)
    extra = jnp.stack([*split3(weight_rows), *split3(target)], axis=1)
    extra = jnp.pad(extra, ((0, 0), (0, LANES - extra.shape[1])))
    unit = jnp.concatenate([inputs, extra.astype(jnp.bfloat16)], axis=1)

    def swap(value, row_bits, col_bits):
        pairs = [
            (r * n_col + c, (r ^ row_bits) * n_col + (c ^ col_bits))
            for r in range(n_row)
            for c in range(n_col)
        ]
        return lax.ppermute(value, ("row", "col"), pairs)

    units = [unit] + [swap(unit, 4 * k, 0) for k in range(1, line)]
    ro = readout.astype(jnp.float32)[None, :]
    fours, rights, strips, mirrors = [], [], [], []
    for k, piece in enumerate(units):
        half = [piece, swap(piece, 0, 1), swap(piece, 2, 0), swap(piece, 2, 1)]
        half = jnp.concatenate(half, axis=0)
        pay = jnp.concatenate([half, swap(half, 1, 0)], axis=0)
        got = stage(k, pay, first_weight, second_weight, ro, fours)
        hid, grad, inn, right, strip = got[:5]
        fours.append((pay, inn, hid, grad))
        rights.append(right)
        strips.append(strip)
        mirrors += got[5:]
    return solve(fours, rights, strips, mirrors, width // (n_row * n_col))


def solution(mesh):
    in_specs = (
        P(("row", "col"), None),
        P(),
        P(),
        P(),
        P(("row", "col")),
        P(("row", "col")),
        P(("row", "col")),
    )
    out_specs = P(("row", "col"), None)
    n_row, n_col = mesh.shape["row"], mesh.shape["col"]

    def body(inputs, *rest):
        rays = inputs.shape[0] * n_row * n_col
        chunk = 8 * inputs.shape[0]
        width = inputs.shape[1]
        held = 4 * rays * rays + 8 * rays * width
        fits = held <= VMEM_BYTES // 2 and n_col == 2 and n_row in (4, 8, 16, 32)
        fits = fits and chunk % SUB == 0 and width % (n_row * n_col * 8) == 0
        return (gathered if fits else shards)(inputs, *rest)

    return jax.shard_map(
        body, mesh=mesh, in_specs=in_specs, out_specs=out_specs, check_vma=False
    )
```

```python
import jax
import jax.numpy as jnp
from jax import lax
from jax.experimental import pallas as pl
from jax.experimental.pallas import tpu as pltpu
from jax.sharding import PartitionSpec as P

VIEWS = 2000
ITERS = 3


DAMP = 4.0
LEARN = 8.0
HIGH = lax.Precision.HIGHEST
LANES = 128
BLOCK = 256
VMEM_BYTES = 30 * 2**20


def slope(value):
    sig = jax.nn.sigmoid(value)
    return sig * (1.0 + value * (1.0 - sig))


def ray_weight(counts, views):
    angle = 2.0 * jnp.pi / VIEWS * views.astype(jnp.float32)
    return counts.astype(jnp.float32) / 16.0 * (1.0 + 0.5 * jnp.cos(angle))


def carry_back(outer_grad, second_weight, pre_first):
    carried = lax.dot_general(
        outer_grad, second_weight, (((1,), (1,)), ((), ())), preferred_element_type=jnp.float32
    )
    return (carried * slope(pre_first)).astype(jnp.bfloat16)


def gram(left, other):
    return lax.dot_general(
        left, other, (((1,), (1,)), ((), ())), preferred_element_type=jnp.float32
    )


def global_sums(values):
    return lax.psum((values[0], values[1]), ("row", "col"))


def shards(inputs, first_weight, second_weight, readout, target, counts, views):
    weight_rows = ray_weight(counts, views)
    pre_first = jnp.dot(inputs, first_weight, preferred_element_type=jnp.float32)
    hidden = jax.nn.silu(pre_first).astype(jnp.bfloat16)
    pre_second = jnp.dot(hidden, second_weight, preferred_element_type=jnp.float32)
    readout_f = readout.astype(jnp.float32)
    signal = jnp.sum(jax.nn.silu(pre_second) * readout_f[None, :], axis=1)
    right = weight_rows * signal - target
    outer_grad = (weight_rows[:, None] * slope(pre_second) * readout_f[None, :]).astype(
        jnp.bfloat16
    )
    inner_grad = carry_back(outer_grad, second_weight, pre_first)
    block_in, block_inner, block_hidden, block_outer = (
        lax.all_gather(inputs, "col", axis=0, tiled=True),
        lax.all_gather(inner_grad, "col", axis=0, tiled=True),
        lax.all_gather(hidden, "col", axis=0, tiled=True),
        lax.all_gather(outer_grad, "col", axis=0, tiled=True),
    )
    cross_in, cross_inner, cross_hidden, cross_outer = (
        lax.all_gather(inputs, "row", axis=0, tiled=True),
        lax.all_gather(inner_grad, "row", axis=0, tiled=True),
        lax.all_gather(hidden, "row", axis=0, tiled=True),
        lax.all_gather(outer_grad, "row", axis=0, tiled=True),
    )
    kernel = gram(block_in, cross_in) * gram(block_inner, cross_inner)
    kernel = kernel + gram(block_hidden, cross_hidden) * gram(block_outer, cross_outer)

    def apply(direction):
        spread = lax.all_gather(direction, "row", axis=0, tiled=True)
        partial_value = jnp.dot(kernel, spread, precision=HIGH, preferred_element_type=jnp.float32)
        own = lax.psum_scatter(partial_value, "col", scatter_dimension=0, tiled=True)
        return own + DAMP * direction

    solution = jnp.zeros_like(right)
    residual = right
    image = apply(residual)
    norm_now, product = global_sums((jnp.sum(residual * residual), jnp.sum(residual * image)))
    alpha = norm_now / product
    direction, along = (residual, image)
    for step in range(ITERS):
        solution = solution + alpha * direction
        residual = residual - alpha * along
        if step + 1 < ITERS:
            image = apply(residual)
            norm_next, product = global_sums(
                (jnp.sum(residual * residual), jnp.sum(residual * image))
            )
            ratio = norm_next / norm_now
            alpha = norm_next / (product - ratio * norm_next / alpha)
            direction = residual + ratio * direction
            along = image + ratio * along
            norm_now = norm_next
    weighted_inner = solution[:, None] * inner_grad.astype(jnp.float32)
    weighted_outer = solution[:, None] * outer_grad.astype(jnp.float32)
    inputs_f = inputs.astype(jnp.float32)
    hidden_f = hidden.astype(jnp.float32)
    first = lax.dot_general(
        inputs_f,
        weighted_inner,
        (((0,), (0,)), ((), ())),
        precision=HIGH,
        preferred_element_type=jnp.float32,
    )
    second = lax.dot_general(
        hidden_f,
        weighted_outer,
        (((0,), (0,)), ((), ())),
        precision=HIGH,
        preferred_element_type=jnp.float32,
    )
    return lax.psum_scatter(
        -LEARN * jnp.concatenate([first, second], axis=1),
        ("row", "col"),
        scatter_dimension=0,
        tiled=True,
    )


def split3(value):
    high = lax.reduce_precision(value, 8, 7)
    rest = value - high
    middle = lax.reduce_precision(rest, 8, 7)
    return high, middle, rest - middle


def bdot(left, right, contract):
    return lax.dot_general(left, right, (contract, ((), ())), preferred_element_type=jnp.float32)


def sigmoid(value):
    return 1.0 / (1.0 + jnp.exp(-value))


def take(refs, start, size, cols):
    parts, offset = [], 0
    for ref in refs:
        low = max(start - offset, 0)
        high = min(start + size - offset, ref.shape[0])
        if low < high:
            parts.append(ref[low:high, cols])
        offset += ref.shape[0]
    return parts[0] if len(parts) == 1 else jnp.concatenate(parts, axis=0)


def features(pays, w1_ref, w2_ref, ro_ref, hid_ref, grad_ref, inn_ref, right_ref):
    rays, width = hid_ref.shape
    extra = take(pays, 0, rays, slice(width, width + LANES)).astype(jnp.float32)
    weight = extra[:, 0:1] + extra[:, 1:2] + extra[:, 2:3]
    target = extra[:, 3:4] + extra[:, 4:5] + extra[:, 5:6]
    pre = bdot(take(pays, 0, rays, slice(0, width)), w1_ref[...], ((1,), (0,)))
    sig = sigmoid(pre)
    slope_first = sig * (1.0 + pre * (1.0 - sig))
    hidden = (pre * sig).astype(jnp.bfloat16)
    hid_ref[...] = hidden
    pre = bdot(hidden, w2_ref[...], ((1,), (0,)))
    sig = sigmoid(pre)
    readout = ro_ref[...]
    signal = jnp.sum(pre * sig * readout, axis=1, keepdims=True)
    grad = (weight * (sig * (1.0 + pre * (1.0 - sig))) * readout).astype(jnp.bfloat16)
    grad_ref[...] = grad
    carried = bdot(grad, w2_ref[...], ((1,), (1,)))
    inn_ref[...] = (carried * slope_first).astype(jnp.bfloat16)
    right_ref[...] = jnp.broadcast_to(weight * signal - target, (rays, LANES))


def products(first, last, pays, inns, hids, grads, strip_ref, mirror_ref):
    width = hids[0].shape[1]
    whole = slice(0, width)
    nt = ((1,), (1,))

    def pair(refs, r, c):
        return bdot(take(refs, r * BLOCK, BLOCK, whole), take(refs, c * BLOCK, BLOCK, whole), nt)

    for r in range(first, last):
        rows = slice((r - first) * BLOCK, (r - first + 1) * BLOCK)
        for c in range(r + 1):
            value = pair(pays, r, c) * pair(inns, r, c) + pair(hids, r, c) * pair(grads, r, c)
            strip_ref[rows, c * BLOCK : (c + 1) * BLOCK] = value
            if c < first:
                mirror_ref[c * BLOCK : (c + 1) * BLOCK, rows] = value.T
            elif c < r:
                other = slice((c - first) * BLOCK, (c - first + 1) * BLOCK)
                strip_ref[other, r * BLOCK : (r + 1) * BLOCK] = value.T


def finish(pays, inns, hids, grads, rights, strips, mirrors, own, out_ref, col_ref):
    width = hids[0].shape[1]
    total = sum(ref.shape[0] for ref in hids)
    tiles = total // LANES

    def to_columns(row):
        for t in range(tiles):
            piece = jnp.broadcast_to(row[:, t * LANES : (t + 1) * LANES], (LANES, LANES))
            col_ref[t * LANES : (t + 1) * LANES, :] = piece.T

    def sweep(ref, offset, pieces, place):
        count = ref.shape[1] // LANES

        def body(g, sums):
            rows = pl.ds(pl.multiple_of(g * 8, 8), 8)
            scale = col_ref[pl.ds(pl.multiple_of(offset + g * 8, 8), 8), :]
            return tuple(
                a + ref[rows, t * LANES : (t + 1) * LANES] * scale for t, a in enumerate(sums)
            )

        zeros = tuple(jnp.zeros((8, LANES), jnp.float32) for _ in range(count))
        for t, a in enumerate(lax.fori_loop(0, ref.shape[0] // 8, body, zeros, unroll=4)):
            k = place + t
            pieces[k] = a if pieces[k] is None else pieces[k] + a

    def apply(row):
        to_columns(row)
        pieces, offset = [None] * tiles, 0
        for strip, mirror in zip(strips, mirrors):
            sweep(strip, offset, pieces, 0)
            if mirror is not None:
                sweep(mirror, 0, pieces, offset // LANES)
            offset += strip.shape[0]
        joined = jnp.concatenate(pieces, axis=1)
        return jnp.sum(joined, axis=0, keepdims=True) + DAMP * row

    def dot(a, b):
        return jnp.sum(a * b, axis=1, keepdims=True)

    right = jnp.concatenate(
        [
            ref[k * LANES : (k + 1) * LANES, :].T[0:1, :]
            for ref in rights
            for k in range(ref.shape[0] // LANES)
        ],
        axis=1,
    )
    answer = jnp.zeros_like(right)
    residual, direction = right, right
    norm_now = dot(right, right)
    for step in range(ITERS):
        image = apply(direction)
        alpha = norm_now / dot(direction, image)
        answer = answer + alpha * direction
        if step + 1 < ITERS:
            residual = residual - alpha * image
            norm_next = dot(residual, residual)
            direction = residual + (norm_next / norm_now) * direction
            norm_now = norm_next
    to_columns(answer)
    rank = lax.axis_index("row") * lax.axis_size("col") + lax.axis_index("col")
    start = rank * own
    base = pl.multiple_of(start // LANES * LANES, LANES)
    shift = (LANES - (start - base)) % LANES
    cols = pl.ds(base, LANES)
    lane = None
    sums = [jnp.zeros((LANES, width), jnp.float32)] * 2
    offset = 0
    for chunk, (inn_ref, grad_ref, hid_ref) in enumerate(zip(inns, grads, hids)):
        rays = hid_ref.shape[0]
        scale = col_ref[offset : offset + rays, :]
        lane = lax.broadcasted_iota(jnp.int32, (rays, LANES), 1)
        lefts = (take(pays, offset, rays, cols), hid_ref[:, cols])
        for which, (left, ref) in enumerate(zip(lefts, (inn_ref, grad_ref))):
            left = pltpu.roll(left.astype(jnp.float32) * scale, shift, 1)
            high = left.astype(jnp.bfloat16).astype(jnp.float32)
            rest = left - high
            middle = rest.astype(jnp.bfloat16).astype(jnp.float32)
            low = rest - middle
            packed = jnp.where(lane < 2 * own, pltpu.roll(middle, own, 1), pltpu.roll(low, 2 * own, 1))
            packed = jnp.where(lane < own, high, packed).astype(jnp.bfloat16)
            sums[which] = sums[which] + bdot(packed, ref[...], ((0,), (0,)))
        offset += rays
    for which, value in enumerate(sums):
        value = value[0:own] + value[own : 2 * own] + value[2 * own : 3 * own]
        out_ref[:, which * width : (which + 1) * width] = -LEARN * value


def stage(k, count, pays, w1, w2, ro, before, own):
    width, units = w1.shape
    rays = sum(a.shape[0] for a in pays)
    first, last = k * rays // BLOCK, (k + 1) * rays // BLOCK
    final = k + 1 == count
    rows, cols = (last - first) * BLOCK, last * BLOCK
    made = [((rays, units), jnp.bfloat16)] * 3 + [((rays, LANES), jnp.float32)]
    made.append(((rows, cols), jnp.float32))
    if first:
        made.append(((first * BLOCK, rows), jnp.float32))
    operands, spots = [], []

    def place(arrays):
        spots.append((len(operands), len(operands) + len(arrays)))
        operands.extend(arrays)

    place([*pays, w1, w2, ro])
    for done in before:
        place(done["pays"])
        place(done["made"] if final else done["made"][:3])

    def kernel(*refs):
        groups = [list(refs[a:b]) for a, b in spots]
        tail = list(refs[len(operands) :])
        out_ref = tail.pop(0) if final else None
        mine = tail[: len(made)]
        own_pays = groups[0][: len(pays)]
        features(own_pays, *groups[0][len(pays) :], *mine[:4])
        old_pays = [ref for group in groups[1::2] for ref in group]
        hids, grads, inns = ([g[i] for g in groups[2::2]] + [mine[i]] for i in range(3))
        every = [*old_pays, *own_pays]
        products(first, last, every, inns, hids, grads, mine[4], mine[5] if first else None)
        if final:
            rights, strips = ([g[i] for g in groups[2::2]] + [mine[i]] for i in (3, 4))
            mirrors = [g[5] if len(g) > 5 else None for g in groups[2::2] + [mine]]
            finish(every, inns, hids, grads, rights, strips, mirrors, own, out_ref, tail[-1])

    vmem = pl.BlockSpec(memory_space=pltpu.VMEM)
    if final:
        out_shape = jax.ShapeDtypeStruct((own, 2 * width), jnp.float32)
        out_specs = vmem
        scratch = [pltpu.VMEM(*m) for m in made]
        scratch.append(pltpu.VMEM((count * rays, LANES), jnp.float32))
    else:
        out_shape = [jax.ShapeDtypeStruct(*m) for m in made]
        out_specs = [vmem] * len(made)
        scratch = []
    flops = 6 * rays * width * units + 4 * width * (last * last - first * first) * BLOCK * BLOCK
    return pl.pallas_call(
        kernel,
        out_shape=out_shape,
        in_specs=[vmem] * len(operands),
        out_specs=out_specs,
        scratch_shapes=scratch,
        cost_estimate=pl.CostEstimate(
            flops=flops, transcendentals=4 * rays * units, bytes_accessed=8 * rays * width
        ),
        compiler_params=pltpu.CompilerParams(vmem_limit_bytes=VMEM_BYTES),
        name=f"stage{k}",
    )(*operands)


def after(value, token):
    return value if token is None else lax.optimization_barrier((value, token))[0]


def gathered(inputs, first_weight, second_weight, readout, target, counts, views):
    n_row, n_col = lax.axis_size("row"), lax.axis_size("col")
    line = n_row // 4
    rays, width = inputs.shape
    weight_rows = ray_weight(counts, views)
    extra = jnp.stack([*split3(weight_rows), *split3(target)], axis=1)
    extra = jnp.pad(extra, ((0, 0), (0, LANES - extra.shape[1])))
    unit = jnp.concatenate([inputs, extra.astype(jnp.bfloat16)], axis=1)

    def swap(value, row_bits, col_bits):
        pairs = [
            (r * n_col + c, (r ^ row_bits) * n_col + (c ^ col_bits))
            for r in range(n_row)
            for c in range(n_col)
        ]
        return lax.ppermute(value, ("row", "col"), pairs)

    units = [unit] + [swap(unit, 4 * k, 0) for k in range(1, line)]
    ro = readout.astype(jnp.float32)[None, :]
    before = []
    for k, piece in enumerate(units):
        half = [piece, swap(piece, 0, 1), swap(piece, 2, 0), swap(piece, 2, 1)]
        half = jnp.concatenate(half, axis=0)
        if k > 1:
            half = after(half, before[k - 2]["made"][3])
        pays = [half, swap(half, 1, 0)]
        got = stage(
            k, line, pays, first_weight, second_weight, ro, before, width // (n_row * n_col)
        )
        before.append({"pays": pays, "made": got})
    return got


def solution(mesh):
    in_specs = (
        P(("row", "col"), None),
        P(),
        P(),
        P(),
        P(("row", "col")),
        P(("row", "col")),
        P(("row", "col")),
    )
    out_specs = P(("row", "col"), None)
    n_row, n_col = mesh.shape["row"], mesh.shape["col"]

    def body(inputs, *rest):
        rays = inputs.shape[0] * n_row * n_col
        chunk = 8 * inputs.shape[0]
        width = inputs.shape[1]
        own = width // (n_row * n_col)
        held = 4 * rays * rays + 8 * rays * width
        fits = held <= VMEM_BYTES and n_col == 2 and n_row in (4, 8, 16, 32)
        fits = fits and chunk % LANES == 0 and chunk >= BLOCK and rays % BLOCK == 0
        fits = fits and width % LANES == 0 and own * n_row * n_col == width
        fits = fits and own % 8 == 0 and LANES % own == 0 and 3 * own <= LANES
        return (gathered if fits else shards)(inputs, *rest)

    return jax.shard_map(
        body, mesh=mesh, in_specs=in_specs, out_specs=out_specs, check_vma=False
    )
```

```python
import jax
import jax.numpy as jnp
from jax import lax
from jax.experimental import pallas as pl
from jax.experimental.pallas import tpu as pltpu
from jax.sharding import PartitionSpec as P


VIEWS = 2000
ITERS = 3


DAMP = 4.0
LEARN = 8.0
HIGH = lax.Precision.HIGHEST
LANES = 128
BLOCK = 256
VMEM_BYTES = 30 * 2**20


def slope(value):
    sig = jax.nn.sigmoid(value)
    return sig * (1.0 + value * (1.0 - sig))


def ray_weight(counts, views):
    angle = 2.0 * jnp.pi / VIEWS * views.astype(jnp.float32)
    return counts.astype(jnp.float32) / 16.0 * (1.0 + 0.5 * jnp.cos(angle))


def carry_back(outer_grad, second_weight, pre_first):
    carried = lax.dot_general(
        outer_grad, second_weight, (((1,), (1,)), ((), ())), preferred_element_type=jnp.float32
    )
    return (carried * slope(pre_first)).astype(jnp.bfloat16)


def gram(left, other):
    return lax.dot_general(
        left, other, (((1,), (1,)), ((), ())), preferred_element_type=jnp.float32
    )


def global_sums(values):
    return lax.psum((values[0], values[1]), ("row", "col"))


def shards(inputs, first_weight, second_weight, readout, target, counts, views):
    weight_rows = ray_weight(counts, views)
    pre_first = jnp.dot(inputs, first_weight, preferred_element_type=jnp.float32)
    hidden = jax.nn.silu(pre_first).astype(jnp.bfloat16)
    pre_second = jnp.dot(hidden, second_weight, preferred_element_type=jnp.float32)
    readout_f = readout.astype(jnp.float32)
    signal = jnp.sum(jax.nn.silu(pre_second) * readout_f[None, :], axis=1)
    right = weight_rows * signal - target
    outer_grad = (weight_rows[:, None] * slope(pre_second) * readout_f[None, :]).astype(
        jnp.bfloat16
    )
    inner_grad = carry_back(outer_grad, second_weight, pre_first)
    block_in, block_inner, block_hidden, block_outer = (
        lax.all_gather(inputs, "col", axis=0, tiled=True),
        lax.all_gather(inner_grad, "col", axis=0, tiled=True),
        lax.all_gather(hidden, "col", axis=0, tiled=True),
        lax.all_gather(outer_grad, "col", axis=0, tiled=True),
    )
    cross_in, cross_inner, cross_hidden, cross_outer = (
        lax.all_gather(inputs, "row", axis=0, tiled=True),
        lax.all_gather(inner_grad, "row", axis=0, tiled=True),
        lax.all_gather(hidden, "row", axis=0, tiled=True),
        lax.all_gather(outer_grad, "row", axis=0, tiled=True),
    )
    kernel = gram(block_in, cross_in) * gram(block_inner, cross_inner)
    kernel = kernel + gram(block_hidden, cross_hidden) * gram(block_outer, cross_outer)

    def apply(direction):
        spread = lax.all_gather(direction, "row", axis=0, tiled=True)
        partial_value = jnp.dot(kernel, spread, precision=HIGH, preferred_element_type=jnp.float32)
        own = lax.psum_scatter(partial_value, "col", scatter_dimension=0, tiled=True)
        return own + DAMP * direction

    solution = jnp.zeros_like(right)
    residual = right
    image = apply(residual)
    norm_now, product = global_sums((jnp.sum(residual * residual), jnp.sum(residual * image)))
    alpha = norm_now / product
    direction, along = (residual, image)
    for step in range(ITERS):
        solution = solution + alpha * direction
        residual = residual - alpha * along
        if step + 1 < ITERS:
            image = apply(residual)
            norm_next, product = global_sums(
                (jnp.sum(residual * residual), jnp.sum(residual * image))
            )
            ratio = norm_next / norm_now
            alpha = norm_next / (product - ratio * norm_next / alpha)
            direction = residual + ratio * direction
            along = image + ratio * along
            norm_now = norm_next
    weighted_inner = solution[:, None] * inner_grad.astype(jnp.float32)
    weighted_outer = solution[:, None] * outer_grad.astype(jnp.float32)
    inputs_f = inputs.astype(jnp.float32)
    hidden_f = hidden.astype(jnp.float32)
    first = lax.dot_general(
        inputs_f,
        weighted_inner,
        (((0,), (0,)), ((), ())),
        precision=HIGH,
        preferred_element_type=jnp.float32,
    )
    second = lax.dot_general(
        hidden_f,
        weighted_outer,
        (((0,), (0,)), ((), ())),
        precision=HIGH,
        preferred_element_type=jnp.float32,
    )
    return lax.psum_scatter(
        -LEARN * jnp.concatenate([first, second], axis=1),
        ("row", "col"),
        scatter_dimension=0,
        tiled=True,
    )


def bdot(left, right, contract):
    return lax.dot_general(left, right, (contract, ((), ())), preferred_element_type=jnp.float32)


def sigmoid(value):
    return 1.0 / (1.0 + jnp.exp(-value))


def take(refs, start, size, cols):
    parts, offset = [], 0
    for ref in refs:
        low = max(start - offset, 0)
        high = min(start + size - offset, ref.shape[0])
        if low < high:
            parts.append(ref[low:high, cols])
        offset += ref.shape[0]
    return parts[0] if len(parts) == 1 else jnp.concatenate(parts, axis=0)


def features(pays, w1_ref, w2_ref, ro_ref, hid_ref, grad_ref, inn_ref, right_ref):
    rays, width = hid_ref.shape
    extra = take(pays, 0, rays, slice(width, width + LANES)).astype(jnp.float32)
    weight = extra[:, 0:1] + extra[:, 1:2] + extra[:, 2:3]
    target = extra[:, 3:4] + extra[:, 4:5] + extra[:, 5:6]
    pre = bdot(take(pays, 0, rays, slice(0, width)), w1_ref[...], ((1,), (0,)))
    sig = sigmoid(pre)
    slope_first = sig * (1.0 + pre * (1.0 - sig))
    hidden = (pre * sig).astype(jnp.bfloat16)
    hid_ref[...] = hidden
    pre = bdot(hidden, w2_ref[...], ((1,), (0,)))
    sig = sigmoid(pre)
    readout = ro_ref[...]
    signal = jnp.sum(pre * sig * readout, axis=1, keepdims=True)
    grad = (weight * (sig * (1.0 + pre * (1.0 - sig))) * readout).astype(jnp.bfloat16)
    grad_ref[...] = grad
    carried = bdot(grad, w2_ref[...], ((1,), (1,)))
    inn_ref[...] = (carried * slope_first).astype(jnp.bfloat16)
    right_ref[...] = jnp.broadcast_to(weight * signal - target, (rays, LANES))


def products(first, last, pays, inns, hids, grads, strip_ref, mirror_ref):
    width = hids[0].shape[1]
    whole = slice(0, width)
    nt = ((1,), (1,))

    def pair(refs, r, c):
        return bdot(take(refs, r * BLOCK, BLOCK, whole), take(refs, c * BLOCK, BLOCK, whole), nt)

    for r in range(first, last):
        rows = slice((r - first) * BLOCK, (r - first + 1) * BLOCK)
        for c in range(r + 1):
            value = pair(pays, r, c) * pair(inns, r, c) + pair(hids, r, c) * pair(grads, r, c)
            strip_ref[rows, c * BLOCK : (c + 1) * BLOCK] = value
            if c < first:
                mirror_ref[c * BLOCK : (c + 1) * BLOCK, rows] = value.T
            elif c < r:
                other = slice((c - first) * BLOCK, (c - first + 1) * BLOCK)
                strip_ref[other, r * BLOCK : (r + 1) * BLOCK] = value.T


def finish(pays, inns, hids, grads, rights, strips, mirrors, own, out_ref, col_ref):
    width = hids[0].shape[1]
    total = sum(ref.shape[0] for ref in hids)
    tiles = total // LANES

    def to_columns(row):
        for t in range(tiles):
            piece = jnp.broadcast_to(row[:, t * LANES : (t + 1) * LANES], (8, LANES)).T
            col_ref[t * LANES : (t + 1) * LANES, :] = jnp.broadcast_to(
                piece[:, 0:1], (LANES, LANES)
            )

    def sweep(ref, offset, pieces, place):
        count = ref.shape[1] // LANES
        groups = ref.shape[0] // 8
        many = 1
        while many * count < 24 and groups % (2 * many) == 0:
            many *= 2

        def body(i, sums):
            terms = [[] for _ in range(count)]
            for j in range(many):
                g = i * many + j
                rows = pl.ds(pl.multiple_of(g * 8, 8), 8)
                scale = col_ref[pl.ds(pl.multiple_of(offset + g * 8, 8), 8), :]
                for t in range(count):
                    terms[t].append(ref[rows, t * LANES : (t + 1) * LANES] * scale)
            for values in terms:
                while len(values) > 1:
                    values[:] = [sum(values[k : k + 2]) for k in range(0, len(values), 2)]
            return tuple(a + values[0] for a, values in zip(sums, terms))

        zeros = tuple(jnp.zeros((8, LANES), jnp.float32) for _ in range(count))
        for t, a in enumerate(lax.fori_loop(0, groups // many, body, zeros, unroll=4)):
            k = place + t
            pieces[k] = a if pieces[k] is None else pieces[k] + a

    def apply(row):
        to_columns(row)
        pieces, offset = [None] * tiles, 0
        for strip, mirror in zip(strips, mirrors):
            sweep(strip, offset, pieces, 0)
            if mirror is not None:
                sweep(mirror, 0, pieces, offset // LANES)
            offset += strip.shape[0]
        joined = jnp.concatenate(pieces, axis=1)
        return jnp.sum(joined, axis=0, keepdims=True) + DAMP * row

    def dot(a, b):
        return jnp.sum(a * b, axis=1, keepdims=True)

    right = jnp.concatenate(
        [
            ref[k * LANES : (k + 1) * LANES, :].T[0:1, :]
            for ref in rights
            for k in range(ref.shape[0] // LANES)
        ],
        axis=1,
    )
    answer = jnp.zeros_like(right)
    residual, direction = right, right
    norm_now = dot(right, right)
    for step in range(ITERS):
        image = apply(direction)
        alpha = norm_now / dot(direction, image)
        answer = answer + alpha * direction
        if step + 1 < ITERS:
            residual = residual - alpha * image
            norm_next = dot(residual, residual)
            direction = residual + (norm_next / norm_now) * direction
            norm_now = norm_next
    to_columns(answer)
    rank = lax.axis_index("row") * lax.axis_size("col") + lax.axis_index("col")
    start = rank * own
    base = pl.multiple_of(start // LANES * LANES, LANES)
    shift = (LANES - (start - base)) % LANES
    cols = pl.ds(base, LANES)
    lane = None
    sums = [jnp.zeros((LANES, width), jnp.float32)] * 2
    offset = 0
    for inn_ref, grad_ref, hid_ref in zip(inns, grads, hids):
        rays = hid_ref.shape[0]
        scale = col_ref[offset : offset + rays, :]
        lane = lax.broadcasted_iota(jnp.int32, (rays, LANES), 1)
        lefts = (take(pays, offset, rays, cols), hid_ref[:, cols])
        for which, (left, ref) in enumerate(zip(lefts, (inn_ref, grad_ref))):
            left = pltpu.roll(left.astype(jnp.float32) * scale, shift, 1)
            high = left.astype(jnp.bfloat16).astype(jnp.float32)
            rest = left - high
            middle = rest.astype(jnp.bfloat16).astype(jnp.float32)
            low = rest - middle
            packed = jnp.where(lane < 2 * own, pltpu.roll(middle, own, 1), pltpu.roll(low, 2 * own, 1))
            packed = jnp.where(lane < own, high, packed).astype(jnp.bfloat16)
            sums[which] = sums[which] + bdot(packed, ref[...], ((0,), (0,)))
        offset += rays
    for which, value in enumerate(sums):
        value = value[0:own] + value[own : 2 * own] + value[2 * own : 3 * own]
        out_ref[:, which * width : (which + 1) * width] = -LEARN * value


def stage(k, count, pays, w1, w2, ro, before, own):
    width, units = w1.shape
    rays = sum(a.shape[0] for a in pays)
    first, last = k * rays // BLOCK, (k + 1) * rays // BLOCK
    final = k + 1 == count
    rows, cols = (last - first) * BLOCK, last * BLOCK
    made = [((rays, units), jnp.bfloat16)] * 3 + [((rays, LANES), jnp.float32)]
    made.append(((rows, cols), jnp.float32))
    if first:
        made.append(((first * BLOCK, rows), jnp.float32))
    operands, spots = [], []

    def place(arrays):
        spots.append((len(operands), len(operands) + len(arrays)))
        operands.extend(arrays)

    place([*pays, w1, w2, ro])
    for done in before:
        place(done["pays"])
        place(done["made"] if final else done["made"][:3])

    def kernel(*refs):
        groups = [list(refs[a:b]) for a, b in spots]
        tail = list(refs[len(operands) :])
        out_ref = tail.pop(0) if final else None
        mine = tail[: len(made)]
        own_pays = groups[0][: len(pays)]
        features(own_pays, *groups[0][len(pays) :], *mine[:4])
        old_pays = [ref for group in groups[1::2] for ref in group]
        hids, grads, inns = ([g[i] for g in groups[2::2]] + [mine[i]] for i in range(3))
        every = [*old_pays, *own_pays]
        products(first, last, every, inns, hids, grads, mine[4], mine[5] if first else None)
        if final:
            rights, strips = ([g[i] for g in groups[2::2]] + [mine[i]] for i in (3, 4))
            mirrors = [g[5] if len(g) > 5 else None for g in groups[2::2] + [mine]]
            finish(every, inns, hids, grads, rights, strips, mirrors, own, out_ref, tail[-1])

    vmem = pl.BlockSpec(memory_space=pltpu.VMEM)
    if final:
        out_shape = jax.ShapeDtypeStruct((own, 2 * width), jnp.float32)
        out_specs = vmem
        scratch = [pltpu.VMEM(*m) for m in made]
        scratch.append(pltpu.VMEM((count * rays, LANES), jnp.float32))
    else:
        out_shape = [jax.ShapeDtypeStruct(*m) for m in made]
        out_specs = [vmem] * len(made)
        scratch = []
    flops = 6 * rays * width * units + 4 * width * (last * last - first * first) * BLOCK * BLOCK
    return pl.pallas_call(
        kernel,
        out_shape=out_shape,
        in_specs=[vmem] * len(operands),
        out_specs=out_specs,
        scratch_shapes=scratch,
        cost_estimate=pl.CostEstimate(
            flops=flops, transcendentals=4 * rays * units, bytes_accessed=8 * rays * width
        ),
        compiler_params=pltpu.CompilerParams(vmem_limit_bytes=VMEM_BYTES),
    )(*operands)


def split3(value):
    high = value.astype(jnp.bfloat16).astype(jnp.float32)
    rest = value - high
    middle = rest.astype(jnp.bfloat16).astype(jnp.float32)
    return high, middle, rest - middle


def table(target, counts, views):
    rays = target.shape[0]

    def kernel(target_ref, counts_ref, views_ref, out_ref):
        rows = [ray_weight(counts_ref[...], views_ref[...]), target_ref[...]]
        rows.append(jnp.zeros((8 - len(rows), rays), jnp.float32))
        out_ref[:, 0:rays] = jnp.concatenate(rows, axis=0)
        out_ref[:, rays:LANES] = jnp.zeros((8, LANES - rays), jnp.float32)

    vmem = pl.BlockSpec(memory_space=pltpu.VMEM)
    return pl.pallas_call(
        kernel,
        out_shape=jax.ShapeDtypeStruct((8, LANES), jnp.float32),
        in_specs=[vmem] * 3,
        out_specs=vmem,
        compiler_params=pltpu.CompilerParams(vmem_limit_bytes=2**20),
        name="table",
    )(target[None, :], counts[None, :], views[None, :])


def join(pieces, tables):
    count = len(pieces)
    rays, width = pieces[0].shape

    def kernel(*refs):
        out_ref = refs[-1]
        for k in range(count):
            rows = slice(k * rays, (k + 1) * rays)
            out_ref[rows, 0:width] = refs[k][...]
            values = refs[count + k][...]
            terms = [*split3(values[0:1, :]), *split3(values[1:2, :])]
            terms.append(jnp.zeros((LANES - len(terms), LANES), jnp.float32))
            square = jnp.concatenate(terms, axis=0).T
            out_ref[rows, width : width + LANES] = square[0:rays, :].astype(jnp.bfloat16)

    vmem = pl.BlockSpec(memory_space=pltpu.VMEM)
    return pl.pallas_call(
        kernel,
        out_shape=jax.ShapeDtypeStruct((count * rays, width + LANES), pieces[0].dtype),
        in_specs=[vmem] * (2 * count),
        out_specs=vmem,
        compiler_params=pltpu.CompilerParams(vmem_limit_bytes=2**21),
        name="join",
    )(*pieces, *tables)


def load(first_weight, second_weight):
    def kernel(a_ref, b_ref, a_out, b_out, sems):
        copies = [
            pltpu.make_async_copy(a_ref, a_out, sems.at[0]),
            pltpu.make_async_copy(b_ref, b_out, sems.at[1]),
        ]
        for copy in copies:
            copy.start()
        for copy in copies:
            copy.wait()

    both = [jax.ShapeDtypeStruct(a.shape, a.dtype) for a in (first_weight, second_weight)]
    return pl.pallas_call(
        kernel,
        out_shape=both,
        in_specs=[pl.BlockSpec(memory_space=pltpu.HBM)] * 2,
        out_specs=[pl.BlockSpec(memory_space=pltpu.VMEM)] * 2,
        scratch_shapes=[pltpu.SemaphoreType.DMA((2,))],
        compiler_params=pltpu.CompilerParams(vmem_limit_bytes=6 * 2**20),
        name="load",
    )(first_weight, second_weight)


def gathered(inputs, first_weight, second_weight, readout, target, counts, views):
    n_row, n_col = lax.axis_size("row"), lax.axis_size("col")
    line = n_row // 4
    _, width = inputs.shape

    def swap(value, moves):
        pairs = []
        for r in range(n_row):
            for c in range(n_col):
                row_bits, col_bits = moves[r % 2]
                pairs.append((r * n_col + c, (r ^ row_bits) * n_col + (c ^ col_bits)))
        return lax.ppermute(value, ("row", "col"), pairs)

    units = [inputs] + [swap(inputs, ((4 * k, 0),) * 2) for k in range(1, line)]
    own_table = table(target, counts, views)
    tables = [own_table]
    tables += [swap(own_table, ((4 * k, 0),) * 2) for k in range(1, line)]
    first_weight, second_weight = load(first_weight, second_weight)
    halves = [join(units, tables)]
    straight, crossed = ((0, 1), (2, 0)), ((2, 0), (0, 1))
    halves.append(swap(halves[0], straight))
    halves.append(swap(halves[0], crossed))
    halves.append(swap(halves[1], crossed))
    ro = readout.astype(jnp.float32)[None, :]
    before = []
    for k, half in enumerate(halves):
        pays = [half, swap(half, ((1, 0),) * 2)]
        got = stage(
            k, len(halves), pays, first_weight, second_weight, ro, before, width // (n_row * n_col)
        )
        before.append({"pays": pays, "made": got})
    return got


def solution(mesh):
    in_specs = (
        P(("row", "col"), None),
        P(),
        P(),
        P(),
        P(("row", "col")),
        P(("row", "col")),
        P(("row", "col")),
    )
    out_specs = P(("row", "col"), None)
    n_row, n_col = mesh.shape["row"], mesh.shape["col"]

    def body(inputs, *rest):
        rays = inputs.shape[0] * n_row * n_col
        chunk = rays // 4
        width = inputs.shape[1]
        own = width // (n_row * n_col)
        held = 4 * rays * rays + 8 * rays * width
        fits = held <= VMEM_BYTES and n_col == 2 and n_row in (4, 8, 16, 32)
        fits = fits and chunk % LANES == 0 and chunk >= BLOCK and rays % BLOCK == 0
        fits = fits and width % LANES == 0 and own * n_row * n_col == width
        fits = fits and own % 8 == 0 and LANES % own == 0 and 3 * own <= LANES
        if not fits:
            return shards(inputs, *rest)
        return gathered(inputs, *rest)

    return jax.shard_map(body, mesh=mesh, in_specs=in_specs, out_specs=out_specs, check_vma=False)
```

```python
import jax
import jax.numpy as jnp
from jax import lax
from jax.experimental import pallas as pl
from jax.experimental.pallas import tpu as pltpu
from jax.sharding import PartitionSpec as P


VIEWS = 2000
ITERS = 3


DAMP = 4.0
LEARN = 8.0
HIGH = lax.Precision.HIGHEST
LANES = 128
BLOCK = 256
VMEM_BYTES = 30 * 2**20


def slope(value):
    sig = jax.nn.sigmoid(value)
    return sig * (1.0 + value * (1.0 - sig))


def ray_weight(counts, views):
    angle = 2.0 * jnp.pi / VIEWS * views.astype(jnp.float32)
    return counts.astype(jnp.float32) / 16.0 * (1.0 + 0.5 * jnp.cos(angle))


def carry_back(outer_grad, second_weight, pre_first):
    carried = lax.dot_general(
        outer_grad, second_weight, (((1,), (1,)), ((), ())), preferred_element_type=jnp.float32
    )
    return (carried * slope(pre_first)).astype(jnp.bfloat16)


def gram(left, other):
    return lax.dot_general(
        left, other, (((1,), (1,)), ((), ())), preferred_element_type=jnp.float32
    )


def global_sums(values):
    return lax.psum((values[0], values[1]), ("row", "col"))


def shards(inputs, first_weight, second_weight, readout, target, counts, views):
    weight_rows = ray_weight(counts, views)
    pre_first = jnp.dot(inputs, first_weight, preferred_element_type=jnp.float32)
    hidden = jax.nn.silu(pre_first).astype(jnp.bfloat16)
    pre_second = jnp.dot(hidden, second_weight, preferred_element_type=jnp.float32)
    readout_f = readout.astype(jnp.float32)
    signal = jnp.sum(jax.nn.silu(pre_second) * readout_f[None, :], axis=1)
    right = weight_rows * signal - target
    outer_grad = (weight_rows[:, None] * slope(pre_second) * readout_f[None, :]).astype(
        jnp.bfloat16
    )
    inner_grad = carry_back(outer_grad, second_weight, pre_first)
    block_in, block_inner, block_hidden, block_outer = (
        lax.all_gather(inputs, "col", axis=0, tiled=True),
        lax.all_gather(inner_grad, "col", axis=0, tiled=True),
        lax.all_gather(hidden, "col", axis=0, tiled=True),
        lax.all_gather(outer_grad, "col", axis=0, tiled=True),
    )
    cross_in, cross_inner, cross_hidden, cross_outer = (
        lax.all_gather(inputs, "row", axis=0, tiled=True),
        lax.all_gather(inner_grad, "row", axis=0, tiled=True),
        lax.all_gather(hidden, "row", axis=0, tiled=True),
        lax.all_gather(outer_grad, "row", axis=0, tiled=True),
    )
    kernel = gram(block_in, cross_in) * gram(block_inner, cross_inner)
    kernel = kernel + gram(block_hidden, cross_hidden) * gram(block_outer, cross_outer)

    def apply(direction):
        spread = lax.all_gather(direction, "row", axis=0, tiled=True)
        partial_value = jnp.dot(kernel, spread, precision=HIGH, preferred_element_type=jnp.float32)
        own = lax.psum_scatter(partial_value, "col", scatter_dimension=0, tiled=True)
        return own + DAMP * direction

    solution = jnp.zeros_like(right)
    residual = right
    image = apply(residual)
    norm_now, product = global_sums((jnp.sum(residual * residual), jnp.sum(residual * image)))
    alpha = norm_now / product
    direction, along = (residual, image)
    for step in range(ITERS):
        solution = solution + alpha * direction
        residual = residual - alpha * along
        if step + 1 < ITERS:
            image = apply(residual)
            norm_next, product = global_sums(
                (jnp.sum(residual * residual), jnp.sum(residual * image))
            )
            ratio = norm_next / norm_now
            alpha = norm_next / (product - ratio * norm_next / alpha)
            direction = residual + ratio * direction
            along = image + ratio * along
            norm_now = norm_next
    weighted_inner = solution[:, None] * inner_grad.astype(jnp.float32)
    weighted_outer = solution[:, None] * outer_grad.astype(jnp.float32)
    inputs_f = inputs.astype(jnp.float32)
    hidden_f = hidden.astype(jnp.float32)
    first = lax.dot_general(
        inputs_f,
        weighted_inner,
        (((0,), (0,)), ((), ())),
        precision=HIGH,
        preferred_element_type=jnp.float32,
    )
    second = lax.dot_general(
        hidden_f,
        weighted_outer,
        (((0,), (0,)), ((), ())),
        precision=HIGH,
        preferred_element_type=jnp.float32,
    )
    return lax.psum_scatter(
        -LEARN * jnp.concatenate([first, second], axis=1),
        ("row", "col"),
        scatter_dimension=0,
        tiled=True,
    )


def bdot(left, right, contract):
    return lax.dot_general(left, right, (contract, ((), ())), preferred_element_type=jnp.float32)


def sigmoid(value):
    return 1.0 / (1.0 + jnp.exp(-value))


def take(refs, start, size, cols):
    parts, offset = [], 0
    for ref in refs:
        low = max(start - offset, 0)
        high = min(start + size - offset, ref.shape[0])
        if low < high:
            parts.append(ref[low:high, cols])
        offset += ref.shape[0]
    return parts[0] if len(parts) == 1 else jnp.concatenate(parts, axis=0)


def features(pays, w1_ref, w2_ref, ro_ref, hid_ref, grad_ref, inn_ref, right_ref):
    rays, width = hid_ref.shape
    extra = take(pays, 0, rays, slice(width, width + LANES)).astype(jnp.float32)
    weight = extra[:, 0:1] + extra[:, 1:2] + extra[:, 2:3]
    target = extra[:, 3:4] + extra[:, 4:5] + extra[:, 5:6]
    pre = bdot(take(pays, 0, rays, slice(0, width)), w1_ref[...], ((1,), (0,)))
    sig = sigmoid(pre)
    slope_first = sig * (1.0 + pre * (1.0 - sig))
    hidden = (pre * sig).astype(jnp.bfloat16)
    hid_ref[...] = hidden
    pre = bdot(hidden, w2_ref[...], ((1,), (0,)))
    sig = sigmoid(pre)
    readout = ro_ref[...]
    signal = jnp.sum(pre * sig * readout, axis=1, keepdims=True)
    grad = (weight * (sig * (1.0 + pre * (1.0 - sig))) * readout).astype(jnp.bfloat16)
    grad_ref[...] = grad
    carried = bdot(grad, w2_ref[...], ((1,), (1,)))
    inn_ref[...] = (carried * slope_first).astype(jnp.bfloat16)
    right_ref[...] = jnp.broadcast_to(weight * signal - target, (rays, LANES))


def products(first, last, pays, inns, hids, grads, strip_ref, mirror_ref):
    width = hids[0].shape[1]
    whole = slice(0, width)
    nt = ((1,), (1,))

    def pair(refs, r, c):
        return bdot(take(refs, r * BLOCK, BLOCK, whole), take(refs, c * BLOCK, BLOCK, whole), nt)

    for r in range(first, last):
        rows = slice((r - first) * BLOCK, (r - first + 1) * BLOCK)
        for c in range(r + 1):
            value = pair(pays, r, c) * pair(inns, r, c) + pair(hids, r, c) * pair(grads, r, c)
            strip_ref[rows, c * BLOCK : (c + 1) * BLOCK] = value
            if c < first:
                mirror_ref[c * BLOCK : (c + 1) * BLOCK, rows] = value.T
            elif c < r:
                other = slice((c - first) * BLOCK, (c - first + 1) * BLOCK)
                strip_ref[other, r * BLOCK : (r + 1) * BLOCK] = value.T


def finish(pays, inns, hids, grads, rights, strips, mirrors, own, out_ref, col_ref):
    width = hids[0].shape[1]
    total = sum(ref.shape[0] for ref in hids)
    tiles = total // LANES

    def to_columns(row):
        for t in range(tiles):
            piece = jnp.broadcast_to(row[:, t * LANES : (t + 1) * LANES], (8, LANES)).T
            col_ref[t * LANES : (t + 1) * LANES, :] = jnp.broadcast_to(
                piece[:, 0:1], (LANES, LANES)
            )

    def sweep(ref, offset, pieces, place):
        count = ref.shape[1] // LANES
        groups = ref.shape[0] // 8
        many = 1
        while many * count < 24 and groups % (2 * many) == 0:
            many *= 2

        def body(i, sums):
            terms = [[] for _ in range(count)]
            for j in range(many):
                g = i * many + j
                rows = pl.ds(pl.multiple_of(g * 8, 8), 8)
                scale = col_ref[pl.ds(pl.multiple_of(offset + g * 8, 8), 8), :]
                for t in range(count):
                    terms[t].append(ref[rows, t * LANES : (t + 1) * LANES] * scale)
            for values in terms:
                while len(values) > 1:
                    values[:] = [sum(values[k : k + 2]) for k in range(0, len(values), 2)]
            return tuple(a + values[0] for a, values in zip(sums, terms))

        zeros = tuple(jnp.zeros((8, LANES), jnp.float32) for _ in range(count))
        for t, a in enumerate(lax.fori_loop(0, groups // many, body, zeros, unroll=4)):
            k = place + t
            pieces[k] = a if pieces[k] is None else pieces[k] + a

    def apply(row):
        pieces, offset = [None] * tiles, 0
        for strip, mirror in zip(strips, mirrors):
            sweep(strip, offset, pieces, 0)
            if mirror is not None:
                sweep(mirror, 0, pieces, offset // LANES)
            offset += strip.shape[0]
        joined = jnp.concatenate(pieces, axis=1)
        return jnp.sum(joined, axis=0, keepdims=True) + DAMP * row

    def dot(a, b):
        return jnp.sum(a * b, axis=1, keepdims=True)

    right = jnp.concatenate(
        [
            ref[k * LANES : (k + 1) * LANES, :].T[0:1, :]
            for ref in rights
            for k in range(ref.shape[0] // LANES)
        ],
        axis=1,
    )
    answer = jnp.zeros_like(right)
    residual, direction = right, right
    norm_now = dot(right, right)
    offset = 0
    for ref in rights:
        col_ref[offset : offset + ref.shape[0], :] = ref[...]
        offset += ref.shape[0]
    for step in range(ITERS):
        if step:
            to_columns(direction)
        image = apply(direction)
        alpha = norm_now / dot(direction, image)
        answer = answer + alpha * direction
        if step + 1 < ITERS:
            residual = residual - alpha * image
            norm_next = dot(residual, residual)
            direction = residual + (norm_next / norm_now) * direction
            norm_now = norm_next
    to_columns(answer)
    rank = lax.axis_index("row") * lax.axis_size("col") + lax.axis_index("col")
    start = rank * own
    base = pl.multiple_of(start // LANES * LANES, LANES)
    shift = (LANES - (start - base)) % LANES
    cols = pl.ds(base, LANES)
    lane = None
    sums = [jnp.zeros((LANES, width), jnp.float32)] * 2
    offset = 0
    for inn_ref, grad_ref, hid_ref in zip(inns, grads, hids):
        rays = hid_ref.shape[0]
        scale = col_ref[offset : offset + rays, :]
        lane = lax.broadcasted_iota(jnp.int32, (rays, LANES), 1)
        lefts = (take(pays, offset, rays, cols), hid_ref[:, cols])
        for which, (left, ref) in enumerate(zip(lefts, (inn_ref, grad_ref))):
            left = pltpu.roll(left.astype(jnp.float32) * scale, shift, 1)
            high = left.astype(jnp.bfloat16).astype(jnp.float32)
            rest = left - high
            middle = rest.astype(jnp.bfloat16).astype(jnp.float32)
            low = rest - middle
            packed = jnp.where(lane < 2 * own, pltpu.roll(middle, own, 1), pltpu.roll(low, 2 * own, 1))
            packed = jnp.where(lane < own, high, packed).astype(jnp.bfloat16)
            sums[which] = sums[which] + bdot(packed, ref[...], ((0,), (0,)))
        offset += rays
    for which, value in enumerate(sums):
        value = value[0:own] + value[own : 2 * own] + value[2 * own : 3 * own]
        out_ref[:, which * width : (which + 1) * width] = -LEARN * value


def stage(k, count, pays, w1, w2, ro, before, own):
    width, units = w1.shape
    rays = sum(a.shape[0] for a in pays)
    first, last = k * rays // BLOCK, (k + 1) * rays // BLOCK
    final = k + 1 == count
    rows, cols = (last - first) * BLOCK, last * BLOCK
    made = [((rays, units), jnp.bfloat16)] * 3 + [((rays, LANES), jnp.float32)]
    made.append(((rows, cols), jnp.float32))
    if first:
        made.append(((first * BLOCK, rows), jnp.float32))
    operands, spots = [], []

    def place(arrays):
        spots.append((len(operands), len(operands) + len(arrays)))
        operands.extend(arrays)

    place([*pays, w1, w2, ro])
    for done in before:
        place(done["pays"])
        place(done["made"] if final else done["made"][:3])

    def kernel(*refs):
        groups = [list(refs[a:b]) for a, b in spots]
        tail = list(refs[len(operands) :])
        out_ref = tail.pop(0) if final else None
        mine = tail[: len(made)]
        own_pays = groups[0][: len(pays)]
        features(own_pays, *groups[0][len(pays) :], *mine[:4])
        old_pays = [ref for group in groups[1::2] for ref in group]
        hids, grads, inns = ([g[i] for g in groups[2::2]] + [mine[i]] for i in range(3))
        every = [*old_pays, *own_pays]
        products(first, last, every, inns, hids, grads, mine[4], mine[5] if first else None)
        if final:
            rights, strips = ([g[i] for g in groups[2::2]] + [mine[i]] for i in (3, 4))
            mirrors = [g[5] if len(g) > 5 else None for g in groups[2::2] + [mine]]
            finish(every, inns, hids, grads, rights, strips, mirrors, own, out_ref, tail[-1])

    vmem = pl.BlockSpec(memory_space=pltpu.VMEM)
    if final:
        out_shape = jax.ShapeDtypeStruct((own, 2 * width), jnp.float32)
        out_specs = vmem
        scratch = [pltpu.VMEM(*m) for m in made]
        scratch.append(pltpu.VMEM((count * rays, LANES), jnp.float32))
    else:
        out_shape = [jax.ShapeDtypeStruct(*m) for m in made]
        out_specs = [vmem] * len(made)
        scratch = []
    flops = 6 * rays * width * units + 4 * width * (last * last - first * first) * BLOCK * BLOCK
    return pl.pallas_call(
        kernel,
        out_shape=out_shape,
        in_specs=[vmem] * len(operands),
        out_specs=out_specs,
        scratch_shapes=scratch,
        cost_estimate=pl.CostEstimate(
            flops=flops, transcendentals=4 * rays * units, bytes_accessed=8 * rays * width
        ),
        compiler_params=pltpu.CompilerParams(vmem_limit_bytes=VMEM_BYTES),
    )(*operands)


def split3(value):
    high = value.astype(jnp.bfloat16).astype(jnp.float32)
    rest = value - high
    middle = rest.astype(jnp.bfloat16).astype(jnp.float32)
    return high, middle, rest - middle


def place_terms(out_ref, start, values, width):
    rays = values.shape[1]
    terms = [*split3(values[0:1, :]), *split3(values[1:2, :])]
    terms.append(jnp.zeros((LANES - len(terms), rays), jnp.float32))
    square = jnp.concatenate(terms, axis=0)
    square = jnp.concatenate([square, jnp.zeros((LANES, LANES - rays), jnp.float32)], axis=1).T
    out_ref[start : start + rays, width : width + LANES] = square[0:rays].astype(jnp.bfloat16)


def join(pieces, tables=()):
    count = len(pieces)
    rows, width = sum(a.shape[0] for a in pieces), pieces[0].shape[1]

    def kernel(*refs):
        out_ref, start = refs[-1], 0
        for k in range(count):
            stop = start + refs[k].shape[0]
            out_ref[start:stop, 0:width] = refs[k][...]
            if tables:
                place_terms(out_ref, start, refs[count + k][...], width)
            start = stop

    vmem = pl.BlockSpec(memory_space=pltpu.VMEM)
    wide = width + LANES if tables else width
    return pl.pallas_call(
        kernel,
        out_shape=jax.ShapeDtypeStruct((rows, wide), pieces[0].dtype),
        in_specs=[vmem] * (count + len(tables)),
        out_specs=vmem,
        compiler_params=pltpu.CompilerParams(vmem_limit_bytes=2**21),
        name="join",
    )(*pieces, *tables)


def load(first_weight, second_weight):
    def kernel(a_ref, b_ref, a_out, b_out, sems):
        copies = [
            pltpu.make_async_copy(a_ref, a_out, sems.at[0]),
            pltpu.make_async_copy(b_ref, b_out, sems.at[1]),
        ]
        for copy in copies:
            copy.start()
        for copy in copies:
            copy.wait()

    both = [jax.ShapeDtypeStruct(a.shape, a.dtype) for a in (first_weight, second_weight)]
    return pl.pallas_call(
        kernel,
        out_shape=both,
        in_specs=[pl.BlockSpec(memory_space=pltpu.HBM)] * 2,
        out_specs=[pl.BlockSpec(memory_space=pltpu.VMEM)] * 2,
        scratch_shapes=[pltpu.SemaphoreType.DMA((2,))],
        compiler_params=pltpu.CompilerParams(vmem_limit_bytes=6 * 2**20),
        name="load",
    )(first_weight, second_weight)


def gathered(inputs, first_weight, second_weight, readout, target, counts, views):
    n_row, n_col = lax.axis_size("row"), lax.axis_size("col")
    line = n_row // 4
    rays, width = inputs.shape

    def swap(value, moves):
        pairs = []
        for r in range(n_row):
            for c in range(n_col):
                row_bits, col_bits = moves[r % 2]
                pairs.append((r * n_col + c, (r ^ row_bits) * n_col + (c ^ col_bits)))
        return lax.ppermute(value, ("row", "col"), pairs)

    first_row = lax.broadcasted_iota(jnp.int32, (2, rays), 0) == 0
    table = jnp.where(first_row, ray_weight(counts, views)[None, :], target[None, :])
    units, tables = [inputs], [table]
    for k in range(1, line):
        units.append(swap(inputs, ((4 * k, 0),) * 2))
        tables.append(swap(table, ((4 * k, 0),) * 2))
    first_weight, second_weight = load(first_weight, second_weight)
    straight, crossed = ((0, 1), (2, 0)), ((2, 0), (0, 1))
    base, one, two, three = [], [], [], []
    for k in range(2):
        some = slice(k * line // 2, (k + 1) * line // 2)
        base.append(join(units[some], tables[some]))
        one.append(swap(base[k], straight))
        two.append(swap(base[k], crossed))
        three.append(swap(one[k], crossed))
    parts = ((base[0], one[0]), (base[1], two[0]), (three[0], one[1]), (three[1], two[1]))
    halves = []
    for both in parts:
        halves.append(join(both))
    ro = readout.astype(jnp.float32)[None, :]
    before = []
    for k, half in enumerate(halves):
        pays = [half, swap(half, ((1, 0),) * 2)]
        got = stage(
            k, len(halves), pays, first_weight, second_weight, ro, before, width // (n_row * n_col)
        )
        before.append({"pays": pays, "made": got})
    return got


def solution(mesh):
    in_specs = (
        P(("row", "col"), None),
        P(),
        P(),
        P(),
        P(("row", "col")),
        P(("row", "col")),
        P(("row", "col")),
    )
    out_specs = P(("row", "col"), None)
    n_row, n_col = mesh.shape["row"], mesh.shape["col"]

    def body(inputs, *rest):
        rays = inputs.shape[0] * n_row * n_col
        chunk = rays // 4
        width = inputs.shape[1]
        own = width // (n_row * n_col)
        held = 4 * rays * rays + 8 * rays * width
        fits = held <= VMEM_BYTES and n_col == 2 and n_row in (8, 16, 32)
        fits = fits and chunk % LANES == 0 and chunk >= BLOCK and rays % BLOCK == 0
        fits = fits and width % LANES == 0 and own * n_row * n_col == width
        fits = fits and own % 8 == 0 and LANES % own == 0 and 3 * own <= LANES
        if not fits:
            return shards(inputs, *rest)
        return gathered(inputs, *rest)

    return jax.shard_map(body, mesh=mesh, in_specs=in_specs, out_specs=out_specs, check_vma=False)
```

```python
import jax
import jax.numpy as jnp
from jax import lax
from jax.experimental import pallas as pl
from jax.experimental.pallas import tpu as pltpu
from jax.sharding import PartitionSpec as P


VIEWS = 2000
ITERS = 3


DAMP = 4.0
LEARN = 8.0
HIGH = lax.Precision.HIGHEST
LANES = 128
BLOCK = 256
VMEM_BYTES = 30 * 2**20


def slope(value):
    sig = jax.nn.sigmoid(value)
    return sig * (1.0 + value * (1.0 - sig))


def ray_weight(counts, views):
    angle = 2.0 * jnp.pi / VIEWS * views.astype(jnp.float32)
    return counts.astype(jnp.float32) / 16.0 * (1.0 + 0.5 * jnp.cos(angle))


def carry_back(outer_grad, second_weight, pre_first):
    carried = lax.dot_general(
        outer_grad, second_weight, (((1,), (1,)), ((), ())), preferred_element_type=jnp.float32
    )
    return (carried * slope(pre_first)).astype(jnp.bfloat16)


def gram(left, other):
    return lax.dot_general(
        left, other, (((1,), (1,)), ((), ())), preferred_element_type=jnp.float32
    )


def global_sums(values):
    return lax.psum((values[0], values[1]), ("row", "col"))


def shards(inputs, first_weight, second_weight, readout, target, counts, views):
    weight_rows = ray_weight(counts, views)
    pre_first = jnp.dot(inputs, first_weight, preferred_element_type=jnp.float32)
    hidden = jax.nn.silu(pre_first).astype(jnp.bfloat16)
    pre_second = jnp.dot(hidden, second_weight, preferred_element_type=jnp.float32)
    readout_f = readout.astype(jnp.float32)
    signal = jnp.sum(jax.nn.silu(pre_second) * readout_f[None, :], axis=1)
    right = weight_rows * signal - target
    outer_grad = (weight_rows[:, None] * slope(pre_second) * readout_f[None, :]).astype(
        jnp.bfloat16
    )
    inner_grad = carry_back(outer_grad, second_weight, pre_first)
    block_in, block_inner, block_hidden, block_outer = (
        lax.all_gather(inputs, "col", axis=0, tiled=True),
        lax.all_gather(inner_grad, "col", axis=0, tiled=True),
        lax.all_gather(hidden, "col", axis=0, tiled=True),
        lax.all_gather(outer_grad, "col", axis=0, tiled=True),
    )
    cross_in, cross_inner, cross_hidden, cross_outer = (
        lax.all_gather(inputs, "row", axis=0, tiled=True),
        lax.all_gather(inner_grad, "row", axis=0, tiled=True),
        lax.all_gather(hidden, "row", axis=0, tiled=True),
        lax.all_gather(outer_grad, "row", axis=0, tiled=True),
    )
    kernel = gram(block_in, cross_in) * gram(block_inner, cross_inner)
    kernel = kernel + gram(block_hidden, cross_hidden) * gram(block_outer, cross_outer)

    def apply(direction):
        spread = lax.all_gather(direction, "row", axis=0, tiled=True)
        partial_value = jnp.dot(kernel, spread, precision=HIGH, preferred_element_type=jnp.float32)
        own = lax.psum_scatter(partial_value, "col", scatter_dimension=0, tiled=True)
        return own + DAMP * direction

    solution = jnp.zeros_like(right)
    residual = right
    image = apply(residual)
    norm_now, product = global_sums((jnp.sum(residual * residual), jnp.sum(residual * image)))
    alpha = norm_now / product
    direction, along = (residual, image)
    for step in range(ITERS):
        solution = solution + alpha * direction
        residual = residual - alpha * along
        if step + 1 < ITERS:
            image = apply(residual)
            norm_next, product = global_sums(
                (jnp.sum(residual * residual), jnp.sum(residual * image))
            )
            ratio = norm_next / norm_now
            alpha = norm_next / (product - ratio * norm_next / alpha)
            direction = residual + ratio * direction
            along = image + ratio * along
            norm_now = norm_next
    weighted_inner = solution[:, None] * inner_grad.astype(jnp.float32)
    weighted_outer = solution[:, None] * outer_grad.astype(jnp.float32)
    inputs_f = inputs.astype(jnp.float32)
    hidden_f = hidden.astype(jnp.float32)
    first = lax.dot_general(
        inputs_f,
        weighted_inner,
        (((0,), (0,)), ((), ())),
        precision=HIGH,
        preferred_element_type=jnp.float32,
    )
    second = lax.dot_general(
        hidden_f,
        weighted_outer,
        (((0,), (0,)), ((), ())),
        precision=HIGH,
        preferred_element_type=jnp.float32,
    )
    return lax.psum_scatter(
        -LEARN * jnp.concatenate([first, second], axis=1),
        ("row", "col"),
        scatter_dimension=0,
        tiled=True,
    )


def bdot(left, right, contract):
    return lax.dot_general(left, right, (contract, ((), ())), preferred_element_type=jnp.float32)


def sigmoid(value):
    return 1.0 / (1.0 + jnp.exp(-value))


def take(refs, start, size, cols):
    parts, offset = [], 0
    for ref in refs:
        low = max(start - offset, 0)
        high = min(start + size - offset, ref.shape[0])
        if low < high:
            parts.append(ref[low:high, cols])
        offset += ref.shape[0]
    return parts[0] if len(parts) == 1 else jnp.concatenate(parts, axis=0)


def features(pays, w1, w2, ro):
    width = w1.shape[0]
    rays = sum(a.shape[0] for a in pays)

    def kernel(*refs):
        pay_refs, (w1_ref, w2_ref, ro_ref, out_ref) = refs[: len(pays)], refs[len(pays) :]
        extra = take(pay_refs, 0, rays, slice(width, width + LANES)).astype(jnp.float32)
        weight = extra[:, 0:1] + extra[:, 1:2] + extra[:, 2:3]
        target = extra[:, 3:4] + extra[:, 4:5] + extra[:, 5:6]
        value = take(pay_refs, 0, rays, slice(0, width))
        out_ref[:, 0:width] = value
        pre = bdot(value, w1_ref[...], ((1,), (0,)))
        sig = sigmoid(pre)
        slope_first = sig * (1.0 + pre * (1.0 - sig))
        hidden = (pre * sig).astype(jnp.bfloat16)
        out_ref[:, 2 * width : 3 * width] = hidden
        pre = bdot(hidden, w2_ref[...], ((1,), (0,)))
        sig = sigmoid(pre)
        readout = ro_ref[...]
        signal = jnp.sum(pre * sig * readout, axis=1, keepdims=True)
        grad = (weight * (sig * (1.0 + pre * (1.0 - sig))) * readout).astype(jnp.bfloat16)
        out_ref[:, 3 * width : 4 * width] = grad
        carried = bdot(grad, w2_ref[...], ((1,), (1,)))
        out_ref[:, width : 2 * width] = (carried * slope_first).astype(jnp.bfloat16)
        terms = split3(weight * signal - target)
        lane = lax.broadcasted_iota(jnp.int32, (rays, LANES), 1)
        spread = jnp.zeros((rays, LANES), jnp.float32)
        for k, term in enumerate(terms):
            spread = jnp.where(lane == k, term, spread)
        out_ref[:, 4 * width : 4 * width + LANES] = spread.astype(jnp.bfloat16)

    vmem = pl.BlockSpec(memory_space=pltpu.VMEM)
    units = w1.shape[1]
    return pl.pallas_call(
        kernel,
        out_shape=jax.ShapeDtypeStruct((rays, 4 * width + LANES), jnp.bfloat16),
        in_specs=[vmem] * (len(pays) + 3),
        out_specs=vmem,
        cost_estimate=pl.CostEstimate(
            flops=6 * rays * width * units,
            transcendentals=4 * rays * units,
            bytes_accessed=8 * rays * width,
        ),
        compiler_params=pltpu.CompilerParams(vmem_limit_bytes=VMEM_BYTES),
        name="features",
    )(*pays, w1, w2, ro)


def products(first, last, width, bundles, strip_ref, mirror_ref):
    nt = ((1,), (1,))

    def pair(k, r, c):
        cols = slice(k * width, (k + 1) * width)
        return bdot(take(bundles, r * BLOCK, BLOCK, cols), take(bundles, c * BLOCK, BLOCK, cols), nt)

    for r in range(first, last):
        rows = slice((r - first) * BLOCK, (r - first + 1) * BLOCK)
        for c in range(r + 1):
            value = pair(0, r, c) * pair(1, r, c) + pair(2, r, c) * pair(3, r, c)
            strip_ref[rows, c * BLOCK : (c + 1) * BLOCK] = value
            if c < first:
                mirror_ref[c * BLOCK : (c + 1) * BLOCK, rows] = value.T
            elif c < r:
                other = slice((c - first) * BLOCK, (c - first + 1) * BLOCK)
                strip_ref[other, r * BLOCK : (r + 1) * BLOCK] = value.T


def finish(width, bundles, strips, mirrors, own, out_ref, col_ref):
    total = sum(ref.shape[0] for ref in bundles)
    tiles = total // LANES

    def to_columns(row):
        for t in range(tiles):
            piece = jnp.broadcast_to(row[:, t * LANES : (t + 1) * LANES], (8, LANES)).T
            col_ref[t * LANES : (t + 1) * LANES, :] = jnp.broadcast_to(
                piece[:, 0:1], (LANES, LANES)
            )

    def sweep(ref, offset, pieces, place):
        count = ref.shape[1] // LANES
        groups = ref.shape[0] // 8
        many = 1
        while many * count < 24 and groups % (2 * many) == 0:
            many *= 2

        def body(i, sums):
            terms = [[] for _ in range(count)]
            for j in range(many):
                g = i * many + j
                rows = pl.ds(pl.multiple_of(g * 8, 8), 8)
                scale = col_ref[pl.ds(pl.multiple_of(offset + g * 8, 8), 8), :]
                for t in range(count):
                    terms[t].append(ref[rows, t * LANES : (t + 1) * LANES] * scale)
            for values in terms:
                while len(values) > 1:
                    values[:] = [sum(values[k : k + 2]) for k in range(0, len(values), 2)]
            return tuple(a + values[0] for a, values in zip(sums, terms))

        zeros = tuple(jnp.zeros((8, LANES), jnp.float32) for _ in range(count))
        for t, a in enumerate(lax.fori_loop(0, groups // many, body, zeros, unroll=4)):
            k = place + t
            pieces[k] = a if pieces[k] is None else pieces[k] + a

    def apply(row):
        pieces, offset = [None] * tiles, 0
        for strip, mirror in zip(strips, mirrors):
            sweep(strip, offset, pieces, 0)
            if mirror is not None:
                sweep(mirror, 0, pieces, offset // LANES)
            offset += strip.shape[0]
        joined = jnp.concatenate(pieces, axis=1)
        return jnp.sum(joined, axis=0, keepdims=True) + DAMP * row

    def dot(a, b):
        return jnp.sum(a * b, axis=1, keepdims=True)

    offset = 0
    for ref in bundles:
        rows = slice(offset, offset + ref.shape[0])
        col_ref[rows, :] = ref[:, 4 * width : 4 * width + LANES].astype(jnp.float32)
        offset += ref.shape[0]
    right = []
    for t in range(tiles):
        square = col_ref[t * LANES : (t + 1) * LANES, :].T
        right.append(square[0:1, :] + square[1:2, :] + square[2:3, :])
    right = jnp.concatenate(right, axis=1)
    answer = jnp.zeros_like(right)
    residual, direction = right, right
    norm_now = dot(right, right)
    for step in range(ITERS):
        to_columns(direction)
        image = apply(direction)
        alpha = norm_now / dot(direction, image)
        answer = answer + alpha * direction
        if step + 1 < ITERS:
            residual = residual - alpha * image
            norm_next = dot(residual, residual)
            direction = residual + (norm_next / norm_now) * direction
            norm_now = norm_next
    to_columns(answer)
    rank = lax.axis_index("row") * lax.axis_size("col") + lax.axis_index("col")
    start = rank * own
    base = pl.multiple_of(start // LANES * LANES, LANES)
    shift = (LANES - (start - base)) % LANES
    lane = lax.broadcasted_iota(jnp.int32, (BLOCK, LANES), 1)
    sums = [jnp.zeros((LANES, width), jnp.float32)] * 2
    for r in range(total // BLOCK):
        scale = col_ref[r * BLOCK : (r + 1) * BLOCK, :]
        for which in range(2):
            cols = pl.ds(pl.multiple_of(base + 2 * which * width, LANES), LANES)
            left = take(bundles, r * BLOCK, BLOCK, cols)
            left = pltpu.roll(left.astype(jnp.float32) * scale, shift, 1)
            high = left.astype(jnp.bfloat16).astype(jnp.float32)
            rest = left - high
            middle = rest.astype(jnp.bfloat16).astype(jnp.float32)
            low = rest - middle
            packed = jnp.where(lane < 2 * own, pltpu.roll(middle, own, 1), pltpu.roll(low, 2 * own, 1))
            packed = jnp.where(lane < own, high, packed).astype(jnp.bfloat16)
            cols = slice((2 * which + 1) * width, (2 * which + 2) * width)
            other = take(bundles, r * BLOCK, BLOCK, cols)
            sums[which] = sums[which] + bdot(packed, other, ((0,), (0,)))
    for which, value in enumerate(sums):
        value = value[0:own] + value[own : 2 * own] + value[2 * own : 3 * own]
        out_ref[:, which * width : (which + 1) * width] = -LEARN * value


def stage(k, count, bundles, before, width, own):
    total = sum(a.shape[0] for a in bundles)
    rays = total // (k + 1)
    first, last = k * rays // BLOCK, (k + 1) * rays // BLOCK
    final = k + 1 == count
    rows = (last - first) * BLOCK
    made = [((rows, last * BLOCK), jnp.float32)]
    if first:
        made.append(((first * BLOCK, rows), jnp.float32))
    old = [a for arrays in before for a in arrays] if final else []
    operands = [*bundles, *old]

    def kernel(*refs):
        every = refs[: len(bundles)]
        earlier = list(refs[len(bundles) : len(operands)])
        tail = list(refs[len(operands) :])
        out_ref = tail.pop(0) if final else None
        strip, mirror = tail[0], tail[1] if first else None
        products(first, last, width, every, strip, mirror)
        if final:
            strips, mirrors = [], []
            for arrays in before:
                strips.append(earlier.pop(0))
                mirrors.append(earlier.pop(0) if len(arrays) > 1 else None)
            finish(width, every, [*strips, strip], [*mirrors, mirror], own, out_ref, tail[-1])

    vmem = pl.BlockSpec(memory_space=pltpu.VMEM)
    if final:
        out_shape = jax.ShapeDtypeStruct((own, 2 * width), jnp.float32)
        out_specs = vmem
        scratch = [pltpu.VMEM(*m) for m in made]
        scratch.append(pltpu.VMEM((total, LANES), jnp.float32))
    else:
        out_shape = [jax.ShapeDtypeStruct(*m) for m in made]
        out_specs = [vmem] * len(made)
        scratch = []
    return pl.pallas_call(
        kernel,
        out_shape=out_shape,
        in_specs=[vmem] * len(operands),
        out_specs=out_specs,
        scratch_shapes=scratch,
        cost_estimate=pl.CostEstimate(
            flops=4 * width * (last * last - first * first) * BLOCK * BLOCK,
            transcendentals=0,
            bytes_accessed=8 * rays * width,
        ),
        compiler_params=pltpu.CompilerParams(vmem_limit_bytes=VMEM_BYTES),
    )(*operands)


def split3(value):
    high = value.astype(jnp.bfloat16).astype(jnp.float32)
    rest = value - high
    middle = rest.astype(jnp.bfloat16).astype(jnp.float32)
    return high, middle, rest - middle


def place_terms(out_ref, start, values, width):
    rays = values.shape[1]
    terms = [*split3(values[0:1, :]), *split3(values[1:2, :])]
    terms.append(jnp.zeros((LANES - len(terms), rays), jnp.float32))
    square = jnp.concatenate(terms, axis=0)
    square = jnp.concatenate([square, jnp.zeros((LANES, LANES - rays), jnp.float32)], axis=1).T
    out_ref[start : start + rays, width : width + LANES] = square[0:rays].astype(jnp.bfloat16)


def join(pieces, tables=()):
    count = len(pieces)
    rows, width = sum(a.shape[0] for a in pieces), pieces[0].shape[1]

    def kernel(*refs):
        out_ref, start = refs[-1], 0
        for k in range(count):
            stop = start + refs[k].shape[0]
            out_ref[start:stop, 0:width] = refs[k][...]
            if tables:
                place_terms(out_ref, start, refs[count + k][...], width)
            start = stop

    vmem = pl.BlockSpec(memory_space=pltpu.VMEM)
    wide = width + LANES if tables else width
    return pl.pallas_call(
        kernel,
        out_shape=jax.ShapeDtypeStruct((rows, wide), pieces[0].dtype),
        in_specs=[vmem] * (count + len(tables)),
        out_specs=vmem,
        compiler_params=pltpu.CompilerParams(vmem_limit_bytes=2**21),
        name="join",
    )(*pieces, *tables)


def load(first_weight, second_weight):
    def kernel(a_ref, b_ref, a_out, b_out, sems):
        copies = [
            pltpu.make_async_copy(a_ref, a_out, sems.at[0]),
            pltpu.make_async_copy(b_ref, b_out, sems.at[1]),
        ]
        for copy in copies:
            copy.start()
        for copy in copies:
            copy.wait()

    both = [jax.ShapeDtypeStruct(a.shape, a.dtype) for a in (first_weight, second_weight)]
    return pl.pallas_call(
        kernel,
        out_shape=both,
        in_specs=[pl.BlockSpec(memory_space=pltpu.HBM)] * 2,
        out_specs=[pl.BlockSpec(memory_space=pltpu.VMEM)] * 2,
        scratch_shapes=[pltpu.SemaphoreType.DMA((2,))],
        compiler_params=pltpu.CompilerParams(vmem_limit_bytes=6 * 2**20),
        name="load",
    )(first_weight, second_weight)


def gathered(inputs, first_weight, second_weight, readout, target, counts, views):
    n_row, n_col = lax.axis_size("row"), lax.axis_size("col")
    line = n_row // 4
    rays, width = inputs.shape

    def swap(value, moves):
        pairs = []
        for r in range(n_row):
            for c in range(n_col):
                row_bits, col_bits = moves[r % 2]
                pairs.append((r * n_col + c, (r ^ row_bits) * n_col + (c ^ col_bits)))
        return lax.ppermute(value, ("row", "col"), pairs)

    first_row = lax.broadcasted_iota(jnp.int32, (2, rays), 0) == 0
    table = jnp.where(first_row, ray_weight(counts, views)[None, :], target[None, :])
    units, tables = [inputs], [table]
    for k in range(1, line):
        units.append(swap(inputs, ((4 * k, 0),) * 2))
        tables.append(swap(table, ((4 * k, 0),) * 2))
    first_weight, second_weight = load(first_weight, second_weight)
    straight, crossed = ((0, 1), (2, 0)), ((2, 0), (0, 1))
    base, one, two, three = [], [], [], []
    for k in range(2):
        some = slice(k * line // 2, (k + 1) * line // 2)
        base.append(join(units[some], tables[some]))
        one.append(swap(base[k], straight))
        two.append(swap(base[k], crossed))
        three.append(swap(one[k], crossed))
    parts = ((base[0], one[0]), (base[1], two[0]), (three[0], one[1]), (three[1], two[1]))
    ro = readout.astype(jnp.float32)[None, :]
    bundles, before = [], []
    for k, both in enumerate(parts):
        mine = features(both, first_weight, second_weight, ro)
        bundles += [mine, swap(mine, ((1, 0),) * 2)]
        before.append(stage(k, len(parts), list(bundles), before, width, width // (n_row * n_col)))
    return before[-1]


def solution(mesh):
    in_specs = (
        P(("row", "col"), None),
        P(),
        P(),
        P(),
        P(("row", "col")),
        P(("row", "col")),
        P(("row", "col")),
    )
    out_specs = P(("row", "col"), None)
    n_row, n_col = mesh.shape["row"], mesh.shape["col"]

    def body(inputs, *rest):
        rays = inputs.shape[0] * n_row * n_col
        chunk = rays // 4
        width = inputs.shape[1]
        own = width // (n_row * n_col)
        held = 4 * rays * rays + 8 * rays * width
        fits = held <= VMEM_BYTES and n_col == 2 and n_row in (8, 16, 32)
        fits = fits and chunk % LANES == 0 and chunk >= BLOCK and rays % BLOCK == 0
        fits = fits and width % LANES == 0 and own * n_row * n_col == width
        fits = fits and own % 8 == 0 and LANES % own == 0 and 3 * own <= LANES
        if not fits:
            return shards(inputs, *rest)
        return gathered(inputs, *rest)

    return jax.shard_map(body, mesh=mesh, in_specs=in_specs, out_specs=out_specs, check_vma=False)
```

```python
import jax
import jax.numpy as jnp
from jax import lax
from jax.experimental import pallas as pl
from jax.experimental.pallas import tpu as pltpu
from jax.sharding import PartitionSpec as P


VIEWS = 2000
ITERS = 3


DAMP = 4.0
LEARN = 8.0
HIGH = lax.Precision.HIGHEST
LANES = 128
BLOCK = 256
VMEM_BYTES = 30 * 2**20


def slope(value):
    sig = jax.nn.sigmoid(value)
    return sig * (1.0 + value * (1.0 - sig))


def ray_weight(counts, views):
    angle = 2.0 * jnp.pi / VIEWS * views.astype(jnp.float32)
    return counts.astype(jnp.float32) / 16.0 * (1.0 + 0.5 * jnp.cos(angle))


def carry_back(outer_grad, second_weight, pre_first):
    carried = lax.dot_general(
        outer_grad, second_weight, (((1,), (1,)), ((), ())), preferred_element_type=jnp.float32
    )
    return (carried * slope(pre_first)).astype(jnp.bfloat16)


def gram(left, other):
    return lax.dot_general(
        left, other, (((1,), (1,)), ((), ())), preferred_element_type=jnp.float32
    )


def global_sums(values):
    return lax.psum((values[0], values[1]), ("row", "col"))


def shards(inputs, first_weight, second_weight, readout, target, counts, views):
    weight_rows = ray_weight(counts, views)
    pre_first = jnp.dot(inputs, first_weight, preferred_element_type=jnp.float32)
    hidden = jax.nn.silu(pre_first).astype(jnp.bfloat16)
    pre_second = jnp.dot(hidden, second_weight, preferred_element_type=jnp.float32)
    readout_f = readout.astype(jnp.float32)
    signal = jnp.sum(jax.nn.silu(pre_second) * readout_f[None, :], axis=1)
    right = weight_rows * signal - target
    outer_grad = (weight_rows[:, None] * slope(pre_second) * readout_f[None, :]).astype(
        jnp.bfloat16
    )
    inner_grad = carry_back(outer_grad, second_weight, pre_first)
    block_in, block_inner, block_hidden, block_outer = (
        lax.all_gather(inputs, "col", axis=0, tiled=True),
        lax.all_gather(inner_grad, "col", axis=0, tiled=True),
        lax.all_gather(hidden, "col", axis=0, tiled=True),
        lax.all_gather(outer_grad, "col", axis=0, tiled=True),
    )
    cross_in, cross_inner, cross_hidden, cross_outer = (
        lax.all_gather(inputs, "row", axis=0, tiled=True),
        lax.all_gather(inner_grad, "row", axis=0, tiled=True),
        lax.all_gather(hidden, "row", axis=0, tiled=True),
        lax.all_gather(outer_grad, "row", axis=0, tiled=True),
    )
    kernel = gram(block_in, cross_in) * gram(block_inner, cross_inner)
    kernel = kernel + gram(block_hidden, cross_hidden) * gram(block_outer, cross_outer)

    def apply(direction):
        spread = lax.all_gather(direction, "row", axis=0, tiled=True)
        partial_value = jnp.dot(kernel, spread, precision=HIGH, preferred_element_type=jnp.float32)
        own = lax.psum_scatter(partial_value, "col", scatter_dimension=0, tiled=True)
        return own + DAMP * direction

    solution = jnp.zeros_like(right)
    residual = right
    image = apply(residual)
    norm_now, product = global_sums((jnp.sum(residual * residual), jnp.sum(residual * image)))
    alpha = norm_now / product
    direction, along = (residual, image)
    for step in range(ITERS):
        solution = solution + alpha * direction
        residual = residual - alpha * along
        if step + 1 < ITERS:
            image = apply(residual)
            norm_next, product = global_sums(
                (jnp.sum(residual * residual), jnp.sum(residual * image))
            )
            ratio = norm_next / norm_now
            alpha = norm_next / (product - ratio * norm_next / alpha)
            direction = residual + ratio * direction
            along = image + ratio * along
            norm_now = norm_next
    weighted_inner = solution[:, None] * inner_grad.astype(jnp.float32)
    weighted_outer = solution[:, None] * outer_grad.astype(jnp.float32)
    inputs_f = inputs.astype(jnp.float32)
    hidden_f = hidden.astype(jnp.float32)
    first = lax.dot_general(
        inputs_f,
        weighted_inner,
        (((0,), (0,)), ((), ())),
        precision=HIGH,
        preferred_element_type=jnp.float32,
    )
    second = lax.dot_general(
        hidden_f,
        weighted_outer,
        (((0,), (0,)), ((), ())),
        precision=HIGH,
        preferred_element_type=jnp.float32,
    )
    return lax.psum_scatter(
        -LEARN * jnp.concatenate([first, second], axis=1),
        ("row", "col"),
        scatter_dimension=0,
        tiled=True,
    )


def bdot(left, right, contract):
    return lax.dot_general(left, right, (contract, ((), ())), preferred_element_type=jnp.float32)


def sigmoid(value):
    return 1.0 / (1.0 + jnp.exp(-value))


def take(refs, start, size, cols):
    parts, offset = [], 0
    for ref in refs:
        low = max(start - offset, 0)
        high = min(start + size - offset, ref.shape[0])
        if low < high:
            parts.append(ref[low:high, cols])
        offset += ref.shape[0]
    return parts[0] if len(parts) == 1 else jnp.concatenate(parts, axis=0)


def features(pays, w1, w2, ro):
    width = w1.shape[0]
    rays = sum(a.shape[0] for a in pays)

    def kernel(*refs):
        pay_refs, (w1_ref, w2_ref, ro_ref, out_ref) = refs[: len(pays)], refs[len(pays) :]
        extra = take(pay_refs, 0, rays, slice(width, width + LANES)).astype(jnp.float32)
        weight = extra[:, 0:1] + extra[:, 1:2] + extra[:, 2:3]
        target = extra[:, 3:4] + extra[:, 4:5] + extra[:, 5:6]
        value = take(pay_refs, 0, rays, slice(0, width))
        out_ref[:, 0:width] = value
        pre = bdot(value, w1_ref[...], ((1,), (0,)))
        sig = sigmoid(pre)
        slope_first = sig * (1.0 + pre * (1.0 - sig))
        hidden = (pre * sig).astype(jnp.bfloat16)
        out_ref[:, 2 * width : 3 * width] = hidden
        pre = bdot(hidden, w2_ref[...], ((1,), (0,)))
        sig = sigmoid(pre)
        readout = ro_ref[...]
        signal = jnp.sum(pre * sig * readout, axis=1, keepdims=True)
        grad = (weight * (sig * (1.0 + pre * (1.0 - sig))) * readout).astype(jnp.bfloat16)
        out_ref[:, 3 * width : 4 * width] = grad
        carried = bdot(grad, w2_ref[...], ((1,), (1,)))
        out_ref[:, width : 2 * width] = (carried * slope_first).astype(jnp.bfloat16)
        terms = split3(weight * signal - target)
        lane = lax.broadcasted_iota(jnp.int32, (rays, LANES), 1)
        spread = jnp.zeros((rays, LANES), jnp.float32)
        for k, term in enumerate(terms):
            spread = jnp.where(lane == k, term, spread)
        out_ref[:, 4 * width : 4 * width + LANES] = spread.astype(jnp.bfloat16)

    vmem = pl.BlockSpec(memory_space=pltpu.VMEM)
    units = w1.shape[1]
    return pl.pallas_call(
        kernel,
        out_shape=jax.ShapeDtypeStruct((rays, 4 * width + LANES), jnp.bfloat16),
        in_specs=[vmem] * (len(pays) + 3),
        out_specs=vmem,
        cost_estimate=pl.CostEstimate(
            flops=6 * rays * width * units,
            transcendentals=4 * rays * units,
            bytes_accessed=8 * rays * width,
        ),
        compiler_params=pltpu.CompilerParams(vmem_limit_bytes=VMEM_BYTES),
        name="features",
    )(*pays, w1, w2, ro)


def products(first, last, width, bundles, strip_ref, mirror_ref):
    nt = ((1,), (1,))

    def pair(k, r, c):
        cols = slice(k * width, (k + 1) * width)
        return bdot(take(bundles, r * BLOCK, BLOCK, cols), take(bundles, c * BLOCK, BLOCK, cols), nt)

    for r in range(first, last):
        rows = slice((r - first) * BLOCK, (r - first + 1) * BLOCK)
        for c in range(r + 1):
            value = pair(0, r, c) * pair(1, r, c) + pair(2, r, c) * pair(3, r, c)
            strip_ref[rows, c * BLOCK : (c + 1) * BLOCK] = value
            if c < first:
                mirror_ref[c * BLOCK : (c + 1) * BLOCK, rows] = value.T
            elif c < r:
                other = slice((c - first) * BLOCK, (c - first + 1) * BLOCK)
                strip_ref[other, r * BLOCK : (r + 1) * BLOCK] = value.T


def finish(width, bundles, strips, mirrors, own, out_ref, col_ref):
    total = sum(ref.shape[0] for ref in bundles)
    tiles = total // LANES

    def to_columns(row):
        for t in range(tiles):
            piece = jnp.broadcast_to(row[:, t * LANES : (t + 1) * LANES], (8, LANES)).T
            col_ref[t * LANES : (t + 1) * LANES, :] = jnp.broadcast_to(
                piece[:, 0:1], (LANES, LANES)
            )

    def sweep(ref, offset, pieces, place):
        count = ref.shape[1] // LANES
        groups = ref.shape[0] // 8
        many = 1
        while many * count < 24 and groups % (2 * many) == 0:
            many *= 2

        def body(i, sums):
            terms = [[] for _ in range(count)]
            for j in range(many):
                g = i * many + j
                rows = pl.ds(pl.multiple_of(g * 8, 8), 8)
                scale = col_ref[pl.ds(pl.multiple_of(offset + g * 8, 8), 8), :]
                for t in range(count):
                    terms[t].append(ref[rows, t * LANES : (t + 1) * LANES] * scale)
            for values in terms:
                while len(values) > 1:
                    values[:] = [sum(values[k : k + 2]) for k in range(0, len(values), 2)]
            return tuple(a + values[0] for a, values in zip(sums, terms))

        zeros = tuple(jnp.zeros((8, LANES), jnp.float32) for _ in range(count))
        for t, a in enumerate(lax.fori_loop(0, groups // many, body, zeros, unroll=4)):
            k = place + t
            pieces[k] = a if pieces[k] is None else pieces[k] + a

    def apply(row):
        pieces, offset = [None] * tiles, 0
        for strip, mirror in zip(strips, mirrors):
            sweep(strip, offset, pieces, 0)
            if mirror is not None:
                sweep(mirror, 0, pieces, offset // LANES)
            offset += strip.shape[0]
        joined = jnp.concatenate(pieces, axis=1)
        return jnp.sum(joined, axis=0, keepdims=True) + DAMP * row

    def dot(a, b):
        return jnp.sum(a * b, axis=1, keepdims=True)

    offset = 0
    for ref in bundles:
        rows = slice(offset, offset + ref.shape[0])
        col_ref[rows, :] = ref[:, 4 * width : 4 * width + LANES].astype(jnp.float32)
        offset += ref.shape[0]
    right = []
    for t in range(tiles):
        square = col_ref[t * LANES : (t + 1) * LANES, :].T
        right.append(square[0:1, :] + square[1:2, :] + square[2:3, :])
    right = jnp.concatenate(right, axis=1)
    answer = jnp.zeros_like(right)
    residual, direction = right, right
    norm_now = dot(right, right)
    for step in range(ITERS):
        to_columns(direction)
        image = apply(direction)
        alpha = norm_now / dot(direction, image)
        answer = answer + alpha * direction
        if step + 1 < ITERS:
            residual = residual - alpha * image
            norm_next = dot(residual, residual)
            direction = residual + (norm_next / norm_now) * direction
            norm_now = norm_next
    to_columns(answer)
    rank = lax.axis_index("row") * lax.axis_size("col") + lax.axis_index("col")
    start = rank * own
    base = pl.multiple_of(start // LANES * LANES, LANES)
    shift = (LANES - (start - base)) % LANES
    lane = lax.broadcasted_iota(jnp.int32, (BLOCK, LANES), 1)
    lefts = [[], []]
    for r in range(total // BLOCK):
        scale = col_ref[r * BLOCK : (r + 1) * BLOCK, :]
        for which in range(2):
            cols = pl.ds(pl.multiple_of(base + 2 * which * width, LANES), LANES)
            left = take(bundles, r * BLOCK, BLOCK, cols)
            left = pltpu.roll(left.astype(jnp.float32) * scale, shift, 1)
            high = left.astype(jnp.bfloat16).astype(jnp.float32)
            rest = left - high
            middle = rest.astype(jnp.bfloat16).astype(jnp.float32)
            low = rest - middle
            packed = jnp.where(lane < 2 * own, pltpu.roll(middle, own, 1), pltpu.roll(low, 2 * own, 1))
            packed = jnp.where(lane < own, high, packed).astype(jnp.bfloat16)
            lefts[which].append(packed)
    for which, left in enumerate(lefts):
        cols = slice((2 * which + 1) * width, (2 * which + 2) * width)
        value = bdot(jnp.concatenate(left, axis=0), take(bundles, 0, total, cols), ((0,), (0,)))
        value = value[0:own] + value[own : 2 * own] + value[2 * own : 3 * own]
        out_ref[:, which * width : (which + 1) * width] = -LEARN * value


def stage(k, count, bundles, before, width, own):
    total = sum(a.shape[0] for a in bundles)
    rays = total // (k + 1)
    first, last = k * rays // BLOCK, (k + 1) * rays // BLOCK
    final = k + 1 == count
    rows = (last - first) * BLOCK
    made = [((rows, last * BLOCK), jnp.float32)]
    if first:
        made.append(((first * BLOCK, rows), jnp.float32))
    old = [a for arrays in before for a in arrays] if final else []
    operands = [*bundles, *old]

    def kernel(*refs):
        every = refs[: len(bundles)]
        earlier = list(refs[len(bundles) : len(operands)])
        tail = list(refs[len(operands) :])
        out_ref = tail.pop(0) if final else None
        strip, mirror = tail[0], tail[1] if first else None
        products(first, last, width, every, strip, mirror)
        if final:
            strips, mirrors = [], []
            for arrays in before:
                strips.append(earlier.pop(0))
                mirrors.append(earlier.pop(0) if len(arrays) > 1 else None)
            finish(width, every, [*strips, strip], [*mirrors, mirror], own, out_ref, tail[-1])

    vmem = pl.BlockSpec(memory_space=pltpu.VMEM)
    if final:
        out_shape = jax.ShapeDtypeStruct((own, 2 * width), jnp.float32)
        out_specs = vmem
        scratch = [pltpu.VMEM(*m) for m in made]
        scratch.append(pltpu.VMEM((total, LANES), jnp.float32))
    else:
        out_shape = [jax.ShapeDtypeStruct(*m) for m in made]
        out_specs = [vmem] * len(made)
        scratch = []
    return pl.pallas_call(
        kernel,
        out_shape=out_shape,
        in_specs=[vmem] * len(operands),
        out_specs=out_specs,
        scratch_shapes=scratch,
        cost_estimate=pl.CostEstimate(
            flops=4 * width * (last * last - first * first) * BLOCK * BLOCK,
            transcendentals=0,
            bytes_accessed=8 * rays * width,
        ),
        compiler_params=pltpu.CompilerParams(vmem_limit_bytes=VMEM_BYTES),
    )(*operands)


def split3(value):
    high = value.astype(jnp.bfloat16).astype(jnp.float32)
    rest = value - high
    middle = rest.astype(jnp.bfloat16).astype(jnp.float32)
    return high, middle, rest - middle


def place_terms(out_ref, start, values, width):
    rays = values.shape[1]
    terms = [*split3(values[0:1, :]), *split3(values[1:2, :])]
    terms.append(jnp.zeros((LANES - len(terms), rays), jnp.float32))
    square = jnp.concatenate(terms, axis=0)
    square = jnp.concatenate([square, jnp.zeros((LANES, LANES - rays), jnp.float32)], axis=1).T
    out_ref[start : start + rays, width : width + LANES] = square[0:rays].astype(jnp.bfloat16)


def join(pieces, tables=()):
    count = len(pieces)
    rows, width = sum(a.shape[0] for a in pieces), pieces[0].shape[1]

    def kernel(*refs):
        out_ref, start = refs[-1], 0
        for k in range(count):
            stop = start + refs[k].shape[0]
            out_ref[start:stop, 0:width] = refs[k][...]
            if tables:
                place_terms(out_ref, start, refs[count + k][...], width)
            start = stop

    vmem = pl.BlockSpec(memory_space=pltpu.VMEM)
    wide = width + LANES if tables else width
    return pl.pallas_call(
        kernel,
        out_shape=jax.ShapeDtypeStruct((rows, wide), pieces[0].dtype),
        in_specs=[vmem] * (count + len(tables)),
        out_specs=vmem,
        compiler_params=pltpu.CompilerParams(vmem_limit_bytes=2**21),
        name="join",
    )(*pieces, *tables)


def load(first_weight, second_weight):
    def kernel(a_ref, b_ref, a_out, b_out, sems):
        copies = [
            pltpu.make_async_copy(a_ref, a_out, sems.at[0]),
            pltpu.make_async_copy(b_ref, b_out, sems.at[1]),
        ]
        for copy in copies:
            copy.start()
        for copy in copies:
            copy.wait()

    both = [jax.ShapeDtypeStruct(a.shape, a.dtype) for a in (first_weight, second_weight)]
    return pl.pallas_call(
        kernel,
        out_shape=both,
        in_specs=[pl.BlockSpec(memory_space=pltpu.HBM)] * 2,
        out_specs=[pl.BlockSpec(memory_space=pltpu.VMEM)] * 2,
        scratch_shapes=[pltpu.SemaphoreType.DMA((2,))],
        compiler_params=pltpu.CompilerParams(vmem_limit_bytes=6 * 2**20),
        name="load",
    )(first_weight, second_weight)


def gathered(inputs, first_weight, second_weight, readout, target, counts, views):
    n_row, n_col = lax.axis_size("row"), lax.axis_size("col")
    line = n_row // 4
    rays, width = inputs.shape

    def swap(value, moves):
        pairs = []
        for r in range(n_row):
            for c in range(n_col):
                row_bits, col_bits = moves[r % 2]
                pairs.append((r * n_col + c, (r ^ row_bits) * n_col + (c ^ col_bits)))
        return lax.ppermute(value, ("row", "col"), pairs)

    first_row = lax.broadcasted_iota(jnp.int32, (2, rays), 0) == 0
    table = jnp.where(first_row, ray_weight(counts, views)[None, :], target[None, :])
    units, tables = [inputs], [table]
    for k in range(1, line):
        units.append(swap(inputs, ((4 * k, 0),) * 2))
        tables.append(swap(table, ((4 * k, 0),) * 2))
    first_weight, second_weight = load(first_weight, second_weight)
    straight, crossed = ((0, 1), (2, 0)), ((2, 0), (0, 1))
    base, one, two, three = [], [], [], []
    for k in range(2):
        some = slice(k * line // 2, (k + 1) * line // 2)
        base.append(join(units[some], tables[some]))
        one.append(swap(base[k], straight))
        two.append(swap(base[k], crossed))
        three.append(swap(one[k], crossed))
    parts = ((base[0], one[0]), (base[1], two[0]), (three[0], one[1]), (three[1], two[1]))
    ro = readout.astype(jnp.float32)[None, :]
    bundles, before = [], []
    for k, both in enumerate(parts):
        mine = features(both, first_weight, second_weight, ro)
        bundles += [mine, swap(mine, ((1, 0),) * 2)]
        before.append(stage(k, len(parts), list(bundles), before, width, width // (n_row * n_col)))
    return before[-1]


def solution(mesh):
    in_specs = (
        P(("row", "col"), None),
        P(),
        P(),
        P(),
        P(("row", "col")),
        P(("row", "col")),
        P(("row", "col")),
    )
    out_specs = P(("row", "col"), None)
    n_row, n_col = mesh.shape["row"], mesh.shape["col"]

    def body(inputs, *rest):
        rays = inputs.shape[0] * n_row * n_col
        chunk = rays // 4
        width = inputs.shape[1]
        own = width // (n_row * n_col)
        held = 4 * rays * rays + 8 * rays * width
        fits = held <= VMEM_BYTES and n_col == 2 and n_row in (8, 16, 32)
        fits = fits and chunk % LANES == 0 and chunk >= BLOCK and rays % BLOCK == 0
        fits = fits and width % LANES == 0 and own * n_row * n_col == width
        fits = fits and own % 8 == 0 and LANES % own == 0 and 3 * own <= LANES
        if not fits:
            return shards(inputs, *rest)
        return gathered(inputs, *rest)

    return jax.shard_map(body, mesh=mesh, in_specs=in_specs, out_specs=out_specs, check_vma=False)
```
